128 devices in a mesh: dp: 16 (over y, z_lo, core), ep: 8 (over z_hi, x).
Axes of the slice: x: 4, y: 4, z: 4 (z_hi: 2, z_lo: 2; z = z_hi * 2 + z_lo), core: 2. Of those that a mesh axis runs over, the one named last changes fastest.
Arguments:
- tokens: bfloat16 [16384, 6144], P(('dp', 'ep')), may hold values from -6 to 6
- out_grad: bfloat16 [16384, 6144], P(('dp', 'ep')), may hold values from -0.75 to 0.75
- expert_ids: int32 [16384, 2], P(('dp', 'ep')), may hold values from 0 to 7, all different within a row; in each aligned block of 128 rows (0 to 127, 128 to 255, ...) at most 40 rows name the same one
- route_weight: float32 [16384, 2], P(('dp', 'ep')), may hold values from 0.2 to 1
- w_gate: bfloat16 [8, 6144, 256], P('ep', 'dp'), may hold values from -0.078125 to 0.078125
- w_up: bfloat16 [8, 6144, 256], P('ep', 'dp'), may hold values from -0.078125 to 0.078125
- w_down: bfloat16 [8, 256, 6144], P('ep', None, 'dp'), may hold values from -0.375 to 0.375
Outputs:
- d_tokens: bfloat16 [16384, 6144], P(('dp', 'ep'))
- grad_gate: float32 [8, 6144, 256], P('ep', 'dp')
- grad_up: float32 [8, 6144, 256], P('ep', 'dp')
- grad_down: float32 [8, 256, 6144], P('ep', None, 'dp')
The draws below stay inside these ranges and needn't reach their ends.
Inputs may be any that keep to these rules, and one draw needn't show every extreme that they name: `expert_ids`: each token names two different experts. Among the 128 tokens of one device (aligned blocks of 128 rows) no expert is named more than 40 times, and in some blocks one expert is named exactly 40 times.
All inputs are finite; a program needn't handle non-finite values.
Results may differ from the reference program's by a relative error of at most 0.0065.
Values may be sent and summed in bfloat16 or wider, within the bound.
A program may use at most 128 MiB of HBM per device.

```python
import math
import jax
import jax.numpy as jnp
import numpy as np
from jax import lax

D = 6144
HIDDEN_SIZE = 256
TOK_DEV = 128
EXPERTS = 8
CAP = 40
TOKENS = 16384


def block_levels(rng, extent, split, smallest, top_value):
    gain = 1.0
    for dim, shards_of in split:
        draws = jax.random.uniform(jax.random.fold_in(jax.random.fold_in(rng, 6), dim), (shards_of,), jnp.float32, smallest / len(split), top_value / len(split))
        gain = gain * jnp.repeat(jnp.exp(draws), extent[dim] // shards_of).reshape((-1,) + (1,) * (len(extent) - 1 - dim))
    return gain


def shared_out(own_key, own, number, rows, count, top, bound, slope):
    order = jax.random.permutation(own_key, count)
    crowded, common = shares(count, rows * top, bound, slope, True), shares(count, rows * top, bound, slope, False)
    places = jnp.arange(count)

    def named(sizes, offset_by):
        used = int((sizes > 0).sum())
        fixed = max(1, used // 4)
        passed = fixed + (places - fixed + offset_by * (used - fixed)) % max(1, count - fixed)
        return jnp.zeros((count,), jnp.int32).at[order[jnp.where(places < fixed, places, passed)]].set(jnp.asarray(sizes, jnp.int32))

    sizes = jnp.where(number % 4 == 0, named(crowded, number // 4), named(common, number - number // 4 - 1))
    mixed = jax.random.permutation(jax.random.fold_in(own, 3), count)
    source_of, receiver = mixed[0:count // 2 * 2:2], mixed[1:count // 2 * 2:2]
    margin = jnp.minimum(sizes[source_of] - 1, bound - sizes[receiver]) // 2
    margin = jnp.where((source_of == order[0]) | (receiver == order[0]) | (sizes[receiver] == 0), 0, jnp.maximum(margin, 0))
    passed = jax.random.randint(jax.random.fold_in(own, 4), (count // 2,), 0, 1 << 20) % (margin + 1)
    sizes = sizes.at[source_of].add(-passed).at[receiver].add(passed)
    items = jnp.searchsorted(jnp.cumsum(sizes), jnp.arange(rows * top), side="right").astype(jnp.int32)
    table = items.reshape(top, rows).T
    table = table[jax.random.permutation(jax.random.fold_in(own, 1), rows)]
    offset_by = jax.random.randint(jax.random.fold_in(own, 2), (rows, 1), 0, top)
    return jnp.take_along_axis(table, (jnp.arange(top)[None, :] + offset_by) % top, axis=1)


def shares(amount, total, limit, slope, full):
    portions = [(1 << 20) // math.isqrt(grade ** slope) + 1 for grade in range(1, amount + 1)]
    largest = limit if full else min(limit, max(-(-total // amount), total * portions[0] // sum(portions)))
    least = 1 if total - largest >= amount - 1 else 0
    given, spare = [largest] + [least] * (amount - 1), total - largest - least * (amount - 1)
    while spare > 0:
        movable = [i for i in range(1, amount) if given[i] < largest] or [i for i in range(1, amount) if given[i] < limit]
        pool, budget = sum([portions[i] for i in movable]), spare
        for i in movable:
            extra = min(limit - given[i], max(1, budget * portions[i] // pool), spare)
            given[i] = given[i] + extra
            spare = spare - extra
    return np.array(given)


def centred(own_key, dims, width, limit, shards=(), kind=jnp.bfloat16):
    result = width * jax.random.normal(own_key, dims, jnp.float32)
    if shards:
        result = result * block_levels(own_key, dims, shards, -0.22, 0.18)
    return jnp.clip(result, -limit, limit).astype(kind)


def setup_inputs(seed: int = 0) -> dict:
    arg_keys = jax.random.split(jax.random.key(seed), 8)
    tokens = centred(arg_keys[0], (TOKENS, D), 1.0, 6.0, ((0, 128),))
    out_grad = centred(arg_keys[1], (TOKENS, D), 0.125, 0.75, ((0, 128),))
    expert_ids_keys = jax.random.split(jax.random.fold_in(arg_keys[2], 1), TOKENS // TOK_DEV)
    expert_ids_turns = jax.random.permutation(jax.random.fold_in(arg_keys[2], 3), TOKENS // TOK_DEV)
    expert_ids = jax.vmap(lambda own, number: shared_out(jax.random.fold_in(arg_keys[2], 2), own, number, TOK_DEV, EXPERTS, 2, CAP, 2))(expert_ids_keys, expert_ids_turns).reshape((TOKENS, 2))
    route_weight = jnp.clip(0.2 + 0.8 * jax.random.uniform(arg_keys[3], (TOKENS, 2), jnp.float32) ** block_levels(arg_keys[3], (TOKENS, 2), ((0, 128),), -0.2, 0.2), 0.2, 1.0)
    w_gate = centred(arg_keys[4], (EXPERTS, D, HIDDEN_SIZE), D ** -0.5, 0.078125, ((0, 8), (1, 16)))
    w_up = centred(arg_keys[5], (EXPERTS, D, HIDDEN_SIZE), D ** -0.5, 0.078125, ((0, 8), (1, 16)))
    w_down = centred(arg_keys[6], (EXPERTS, HIDDEN_SIZE, D), HIDDEN_SIZE ** -0.5, 0.375, ((0, 8), (2, 16)))
    return dict(tokens=tokens, out_grad=out_grad, expert_ids=expert_ids, route_weight=route_weight, w_gate=w_gate, w_up=w_up, w_down=w_down)


def slot_rank(flat_ids):
    onehot = (flat_ids[..., None] == jnp.arange(EXPERTS, dtype=jnp.int32)).astype(jnp.int32)
    before = jnp.cumsum(onehot, axis=1) - onehot
    return jnp.sum(before * onehot, axis=-1)


def expert_backward(x_rows, scaled, gate_w, up_w, down_w):
    gate_pre = jnp.dot(x_rows, gate_w, preferred_element_type=jnp.float32)
    up_pre = jnp.dot(x_rows, up_w, preferred_element_type=jnp.float32)
    grad_hidden = lax.dot_general(scaled, down_w, (((1,), (1,)), ((), ())), preferred_element_type=jnp.float32)
    sigmoid_a = jax.nn.sigmoid(gate_pre)
    silu_a = gate_pre * sigmoid_a
    hidden = (silu_a * up_pre).astype(jnp.bfloat16)
    grad_gate_pre = (grad_hidden * up_pre * sigmoid_a * (1.0 + gate_pre * (1.0 - sigmoid_a))).astype(jnp.bfloat16)
    grad_up_pre = (grad_hidden * silu_a).astype(jnp.bfloat16)
    grad_rows = lax.dot_general(grad_gate_pre, gate_w, (((1,), (1,)), ((), ())), preferred_element_type=jnp.float32)
    grad_rows = grad_rows + lax.dot_general(grad_up_pre, up_w, (((1,), (1,)), ((), ())), preferred_element_type=jnp.float32)
    return grad_rows.astype(jnp.bfloat16), grad_gate_pre, grad_up_pre, hidden


def reference(tokens, out_grad, expert_ids, route_weight, w_gate, w_up, w_down):
    blocks = TOKENS // TOK_DEV
    per_expert = blocks * CAP
    ranks_all = slot_rank(expert_ids.reshape(blocks, 2 * TOK_DEV)).reshape(TOKENS, 2)
    block_of = (jnp.arange(TOKENS, dtype=jnp.int32) // TOK_DEV)[:, None]
    slot_index = (expert_ids * per_expert + block_of * CAP + ranks_all).reshape(-1).astype(jnp.int32)
    slot_source = jnp.full((EXPERTS * per_expert,), 2 * TOKENS, jnp.int32)
    slot_source = slot_source.at[slot_index].set(jnp.arange(2 * TOKENS, dtype=jnp.int32))
    flat_weight = route_weight.reshape(-1)

    def one_expert(inputs):
        expert, gate_w, up_w, down_w = inputs
        source = lax.dynamic_slice_in_dim(slot_source, (expert * per_expert).astype(jnp.int32), per_expert)
        filled = source < 2 * TOKENS
        clamped = jnp.minimum(source, 2 * TOKENS - 1)
        token_row = clamped // 2
        x_rows = jnp.where(filled[:, None], tokens[token_row], jnp.zeros((), tokens.dtype))
        weight_rows = jnp.where(filled, flat_weight[clamped], jnp.zeros((), flat_weight.dtype))
        scaled = (weight_rows[:, None] * out_grad[token_row].astype(jnp.float32)).astype(jnp.bfloat16)
        grad_rows, grad_gate_pre, grad_up_pre, hidden = expert_backward(x_rows, scaled, gate_w, up_w, down_w)
        grad_gate = lax.dot_general(x_rows, grad_gate_pre, (((0,), (0,)), ((), ())), preferred_element_type=jnp.float32)
        grad_up = lax.dot_general(x_rows, grad_up_pre, (((0,), (0,)), ((), ())), preferred_element_type=jnp.float32)
        grad_down = lax.dot_general(hidden, scaled, (((0,), (0,)), ((), ())), preferred_element_type=jnp.float32)
        return grad_rows, grad_gate, grad_up, grad_down

    grad_rows, grad_gate, grad_up, grad_down = lax.map(
        one_expert, (jnp.arange(EXPERTS, dtype=jnp.int32), w_gate, w_up, w_down))
    picked = grad_rows.reshape(-1, D)[slot_index].reshape(TOKENS, 2, D)
    d_tokens = jnp.sum(picked.astype(jnp.float32), axis=1).astype(jnp.bfloat16)
    return d_tokens, grad_gate, grad_up, grad_down
```

```python
import functools

import jax
import jax.numpy as jnp
from jax import lax
from jax.experimental import pallas as pl
from jax.experimental.pallas import tpu as pltpu
from jax.sharding import PartitionSpec as P

MESH = pl.DeviceIdType.MESH
F32, BF16 = jnp.float32, jnp.bfloat16
PEERS = [(dy, dz) for dy in (2, 1, 3, 0) for dz in (1, 0) if (dy, dz) != (0, 0)]


class Spot:
    def __init__(self):
        dp, ep = lax.axis_index("dp"), lax.axis_index("ep")
        self.y, self.zl, self.c = dp // 4, (dp // 2) % 2, dp % 2
        self.zh, self.x = ep // 4, ep % 4
        self.q = dp // 2

    def to(self, y=0, zl=0, c=0, zh=0, x=0):
        dp = (self.y + y) % 4 * 4 + (self.zl + zl) % 2 * 2 + (self.c + c) % 2
        return (dp, (self.zh + zh) % 2 * 4 + (self.x + x) % 4)

    def block(self, y, zl):
        return (self.y + y) % 4 * 2 + (self.zl + zl) % 2

    def expert(self, x, zh):
        return (self.zh + zh) % 2 * 4 + (self.x + x) % 4


class Links:
    def __init__(self, send_sem, recv_sem):
        self.send_sem, self.recv_sem, self.count, self.sent = send_sem, recv_sem, 0, []

    def send(self, src, dst, device):
        n = self.count
        self.count += 1
        copy = pltpu.make_async_remote_copy(
            src_ref=src,
            dst_ref=dst,
            send_sem=self.send_sem.at[n],
            recv_sem=self.recv_sem.at[n],
            device_id=device,
            device_id_type=MESH,
        )
        copy.start()
        self.sent.append(copy)
        return copy

    def finish(self):
        for copy in self.sent:
            copy.wait_send()


def greet(devices):
    barrier = pltpu.get_barrier_semaphore()
    for device in devices:
        pl.semaphore_signal(barrier, inc=1, device_id=device, device_id_type=MESH)
    pl.semaphore_wait(barrier, len(devices))


def add_rows(dst, sources, rows, step=32):
    @pl.loop(0, rows // step)
    def _(i):
        at = pl.ds(pl.multiple_of(i * step, step), step)
        total = sources[0][at, :].astype(F32)
        for source in sources[1:]:
            total = total + source[at, :].astype(F32)
        dst[at, :] = total.astype(dst.dtype)


SPREAD_COPIES = 21 + 1 + 2 + 1 + 3 + 6 + 6 + 4


def spread_kernel(tok, og, ids, w_in, x_out, og_out, ids_out, w_out, send_sem, recv_sem, own_sem):
    me = Spot()
    right, left, core, far = me.to(x=1), me.to(x=3), me.to(c=1), me.to(zh=1)
    greet([me.to(y=dy, zl=dz) for dy, dz in PEERS] + [right, left, core, far])
    links = Links(send_sem, recv_sem)
    own, far_e = me.expert(0, 0), me.expert(0, 1)

    from_far = links.send(w_in, w_out.at[own, me.c], far)
    from_left0 = links.send(w_in, w_out.at[own, me.c], right)
    from_right0 = links.send(w_in, w_out.at[own, me.c], left)
    columns = []
    for dy, dz in PEERS:
        there, device = me.block(dy, dz), me.to(y=dy, zl=dz)
        cols = pl.ds(pl.multiple_of(there * 768, 768), 768)
        columns.append(links.send(tok.at[:, cols], x_out.at[me.q], device))
        columns.append(links.send(og.at[:, cols], og_out.at[me.q], device))
        columns.append(links.send(ids, ids_out.at[me.q], device))
    from_core = [links.send(w_in, w_out.at[own, me.c], core)]
    cols = pl.ds(pl.multiple_of(me.q * 768, 768), 768)
    local = [
        pltpu.make_async_copy(w_in, w_out.at[own, me.c], own_sem.at[0]),
        pltpu.make_async_copy(tok.at[:, cols], x_out.at[me.q], own_sem.at[1]),
        pltpu.make_async_copy(og.at[:, cols], og_out.at[me.q], own_sem.at[2]),
        pltpu.make_async_copy(ids, ids_out.at[me.q], own_sem.at[3]),
    ]
    for copy in local:
        copy.start()

    def pass_on(expert, device, rows=pl.ds(0, 384)):
        piece = w_out.at[expert, me.c, rows, :]
        return links.send(piece, piece, device)

    low, high = pl.ds(0, 192), pl.ds(192, 192)
    from_far.wait_recv()
    from_left1 = pass_on(far_e, right)
    from_right1 = pass_on(far_e, left)
    from_core.append(pass_on(far_e, core))
    halves = []
    for dz, from_left, from_right in ((0, from_left0, from_right0), (1, from_left1, from_right1)):
        from_left.wait_recv()
        halves.append(pass_on(me.expert(3, dz), right, low))
        from_core.append(pass_on(me.expert(3, dz), core))
        from_right.wait_recv()
        halves.append(pass_on(me.expert(1, dz), left, high))
        from_core.append(pass_on(me.expert(1, dz), core))
    for n, half in enumerate(halves):
        half.wait_recv()
        from_core.append(pass_on(me.expert(2, n // 2), core, (low, high)[n % 2]))
    for copy in columns + from_core:
        copy.wait_recv()
    for copy in local:
        copy.wait()
    links.finish()


def spread(tokens, out_grad, ids, w_cat):
    vmem, anywhere = pl.BlockSpec(memory_space=pltpu.VMEM), pl.BlockSpec(memory_space=pl.ANY)
    return pl.pallas_call(
        spread_kernel,
        out_shape=(
            jax.ShapeDtypeStruct((8, 128, 768), BF16),
            jax.ShapeDtypeStruct((8, 128, 768), BF16),
            jax.ShapeDtypeStruct((8, 8, 128), jnp.int32),
            jax.ShapeDtypeStruct((8, 2, 384, 768), BF16),
        ),
        in_specs=[vmem] * 4,
        out_specs=(anywhere,) * 4,
        scratch_shapes=[
            pltpu.SemaphoreType.DMA((SPREAD_COPIES,)),
            pltpu.SemaphoreType.DMA((SPREAD_COPIES,)),
            pltpu.SemaphoreType.DMA((4,)),
        ],
        compiler_params=pltpu.CompilerParams(collective_id=0, has_side_effects=True),
        name="spread",
    )(tokens, out_grad, ids, w_cat)


def activation(pre, weight):
    gate, up, grad_hidden = pre[:, :256], pre[:, 256:512], pre[:, 512:] * weight
    sig = jax.nn.sigmoid(gate)
    silu = gate * sig
    hidden = silu * up * weight
    grad_gate = grad_hidden * up * sig * (1.0 + gate * (1.0 - sig))
    grad_up = grad_hidden * silu
    return grad_gate.astype(BF16), grad_up.astype(BF16), hidden.astype(BF16)


MIDDLE_COPIES = 8 + 4 + 1 + 3 + 2 + 4


def middle_kernel(part, weight, h_out, ra, rb, sa, sb, fl, fr, zs, zr, own, send_sem, recv_sem, own_sem):
    me = Spot()
    right, left, pair = me.to(y=1), me.to(y=3), me.to(zl=1)
    greet([right, left, pair])
    links = Links(send_sem, recv_sem)
    low, high = pl.ds(0, 128), pl.ds(128, 128)

    first_a, first_b, other_b, other_a, last_a, last_b = {}, {}, {}, {}, {}, {}
    for dz in (1, 0):
        first_a[dz] = links.send(part.at[me.block(2, dz), low, :], ra.at[dz], right)
        first_b[dz] = links.send(part.at[me.block(2, dz), high, :], rb.at[dz], left)
    for dz in (1, 0):
        other_b[dz] = links.send(part.at[me.block(1, dz), high, :], fl.at[dz, high, :], right)
        other_a[dz] = links.send(part.at[me.block(3, dz), low, :], fr.at[dz, low, :], left)
    for dz in (1, 0):
        first_a[dz].wait_recv()
        add_rows(sa.at[dz], [part.at[me.block(1, dz), low, :], ra.at[dz]], 128)
        last_a[dz] = links.send(sa.at[dz], fl.at[dz, low, :], right)
        first_b[dz].wait_recv()
        add_rows(sb.at[dz], [part.at[me.block(3, dz), high, :], rb.at[dz]], 128)
        last_b[dz] = links.send(sb.at[dz], fr.at[dz, high, :], left)
    for group in (other_b, other_a, last_a, last_b):
        group[1].wait_recv()
    add_rows(zs, [part.at[me.block(0, 1)], fl.at[1], fr.at[1]], 256)
    cross = links.send(zs, zr, pair)
    for group in (other_b, other_a, last_a, last_b):
        group[0].wait_recv()
    cross.wait_recv()

    @pl.loop(0, 16)
    def _(i):
        at = pl.ds(pl.multiple_of(i * 16, 16), 16)
        pre = part[me.block(0, 0), at, :].astype(F32) + zr[at, :].astype(F32)
        pre = pre + fl[0, at, :].astype(F32) + fr[0, at, :].astype(F32)
        own[at, :256], own[at, 256:512], own[at, 512:] = activation(pre, weight[at, :])

    mine = pltpu.make_async_copy(own, h_out.at[me.q], own_sem)
    mine.start()
    from_pair = links.send(own, h_out.at[me.q], pair)
    from_left0 = links.send(own, h_out.at[me.q], right)
    from_right0 = links.send(own, h_out.at[me.q], left)

    def pass_on(block, device, rows=pl.ds(0, 256)):
        piece = h_out.at[block, rows, :]
        return links.send(piece, piece, device)

    from_pair.wait_recv()
    from_left1 = pass_on(me.block(0, 1), right)
    from_right1 = pass_on(me.block(0, 1), left)
    halves = []
    for dz, from_left, from_right in ((0, from_left0, from_right0), (1, from_left1, from_right1)):
        from_left.wait_recv()
        halves.append(pass_on(me.block(3, dz), right, low))
        from_right.wait_recv()
        halves.append(pass_on(me.block(1, dz), left, high))
    for half in halves:
        half.wait_recv()
    mine.wait()
    links.finish()


def middle(part, weight):
    vmem, anywhere = pl.BlockSpec(memory_space=pltpu.VMEM), pl.BlockSpec(memory_space=pl.ANY)
    half, full = pltpu.VMEM((2, 128, 768), BF16), pltpu.VMEM((2, 256, 768), BF16)
    one = pltpu.VMEM((256, 768), BF16)
    return pl.pallas_call(
        middle_kernel,
        out_shape=jax.ShapeDtypeStruct((8, 256, 768), BF16),
        in_specs=[vmem] * 2,
        out_specs=anywhere,
        scratch_shapes=[half] * 4 + [full] * 2 + [one] * 3 + [
            pltpu.SemaphoreType.DMA((MIDDLE_COPIES,)),
            pltpu.SemaphoreType.DMA((MIDDLE_COPIES,)),
            pltpu.SemaphoreType.DMA,
        ],
        compiler_params=pltpu.CompilerParams(collective_id=1, has_side_effects=True),
        name="middle",
    )(part, weight)


COLLECT_COPIES = 7 + 8 + 4 + 4 + 4 + 1


def collect_kernel(dx, g, d_out, g_out, cr, a2, ra, rb, sa, sb, oa, ob, fl, fr, zs, zr, send_sem, recv_sem, own_sem):
    me = Spot()
    right, left, core, far = me.to(x=1), me.to(x=3), me.to(c=1), me.to(zh=1)
    greet([me.to(y=dy, zl=dz) for dy, dz in PEERS] + [right, left, core, far])
    links = Links(send_sem, recv_sem)
    low, high = pl.ds(0, 192), pl.ds(192, 192)
    mine, others = me.c, 1 - me.c

    swapped = {}
    for step, dz in ((2, 1), (2, 0), (1, 1), (3, 1), (1, 0), (3, 0), (0, 1), (0, 0)):
        e = me.expert(step, dz)
        swapped[step, dz] = links.send(g.at[e, others], cr.at[e], core)
    back = []
    cols = pl.ds(pl.multiple_of(me.q * 768, 768), 768)
    for dy, dz in PEERS:
        back.append(links.send(dx.at[me.block(dy, dz)], d_out.at[:, cols], me.to(y=dy, zl=dz)))
    keep = pltpu.make_async_copy(dx.at[me.q], d_out.at[:, cols], own_sem)
    keep.start()

    first_a, first_b, other_b, other_a, last_a, last_b = {}, {}, {}, {}, {}, {}
    for dz in (1, 0):
        e = me.expert(2, dz)
        swapped[2, dz].wait_recv()
        add_rows(a2.at[dz], [g.at[e, mine], cr.at[e]], 384)
        first_a[dz] = links.send(a2.at[dz, low, :], ra.at[dz], right)
        first_b[dz] = links.send(a2.at[dz, high, :], rb.at[dz], left)
    for dz in (1, 0):
        e = me.expert(1, dz)
        swapped[1, dz].wait_recv()
        add_rows(ob.at[dz], [g.at[e, mine, high, :], cr.at[e, high, :]], 192)
        other_b[dz] = links.send(ob.at[dz], fl.at[dz, high, :], right)
        e = me.expert(3, dz)
        swapped[3, dz].wait_recv()
        add_rows(oa.at[dz], [g.at[e, mine, low, :], cr.at[e, low, :]], 192)
        other_a[dz] = links.send(oa.at[dz], fr.at[dz, low, :], left)
    for dz in (1, 0):
        e = me.expert(1, dz)
        first_a[dz].wait_recv()
        add_rows(sa.at[dz], [g.at[e, mine, low, :], cr.at[e, low, :], ra.at[dz]], 192)
        last_a[dz] = links.send(sa.at[dz], fl.at[dz, low, :], right)
        e = me.expert(3, dz)
        first_b[dz].wait_recv()
        add_rows(sb.at[dz], [g.at[e, mine, high, :], cr.at[e, high, :], rb.at[dz]], 192)
        last_b[dz] = links.send(sb.at[dz], fr.at[dz, high, :], left)
    for group in (other_b, other_a, last_a, last_b):
        group[1].wait_recv()
    e = me.expert(0, 1)
    swapped[0, 1].wait_recv()
    add_rows(zs, [g.at[e, mine], cr.at[e], fl.at[1], fr.at[1]], 384)
    cross = links.send(zs, zr, far)
    for group in (other_b, other_a, last_a, last_b):
        group[0].wait_recv()
    swapped[0, 0].wait_recv()
    cross.wait_recv()
    e = me.expert(0, 0)
    add_rows(g_out, [g.at[e, mine], cr.at[e], fl.at[0], fr.at[0], zr], 384)
    for copy in back:
        copy.wait_recv()
    keep.wait()
    links.finish()


def collect(dx, g):
    vmem, anywhere = pl.BlockSpec(memory_space=pltpu.VMEM), pl.BlockSpec(memory_space=pl.ANY)
    half, full = pltpu.VMEM((2, 192, 768), BF16), pltpu.VMEM((2, 384, 768), BF16)
    one = pltpu.VMEM((384, 768), BF16)
    return pl.pallas_call(
        collect_kernel,
        out_shape=(
            jax.ShapeDtypeStruct((128, 6144), BF16),
            jax.ShapeDtypeStruct((384, 768), F32),
        ),
        in_specs=[vmem] * 2,
        out_specs=(anywhere, vmem),
        scratch_shapes=[pltpu.VMEM((8, 384, 768), BF16), full] + [half] * 6 + [full] * 2 + [one] * 2 + [
            pltpu.SemaphoreType.DMA((COLLECT_COPIES,)),
            pltpu.SemaphoreType.DMA((COLLECT_COPIES,)),
            pltpu.SemaphoreType.DMA,
        ],
        compiler_params=pltpu.CompilerParams(collective_id=2, has_side_effects=True, vmem_limit_bytes=50 << 20),
        name="collect",
    )(dx, g)


def nt(left, right):
    return lax.dot_general(left, right, (((1,), (1,)), ((), ())), preferred_element_type=F32)


def tn(left, right):
    return lax.dot_general(left, right, (((0,), (0,)), ((), ())), preferred_element_type=F32)


def partial_pre(x, og, ids_all, w):
    total = [jnp.zeros((1024, 768), F32) for _ in range(2)]
    for e in range(8):
        y = jnp.concatenate(
            [
                jnp.dot(x, w[e, :, :512], preferred_element_type=F32),
                jnp.dot(og, w[e, :, 512:], preferred_element_type=F32),
            ],
            axis=1,
        )
        for k in range(2):
            total[k] = jnp.where(ids_all[:, k : k + 1] == e, y, total[k])
    both = jnp.stack([t.reshape(8, 128, 768) for t in total], axis=1)
    return both.reshape(8, 256, 768).astype(BF16)


def backward(x, og, ids_all, w, h):
    h = h.reshape(8, 2, 128, 768)
    zero = jnp.zeros((), BF16)
    ids_b = ids_all.reshape(8, 128, 2)
    dx = jnp.zeros((1024, 768), F32)
    grads = []
    for e in range(8):
        he = jnp.where(ids_b[:, :, 0:1] == e, h[:, 0], zero)
        he = jnp.where(ids_b[:, :, 1:2] == e, h[:, 1], he).reshape(1024, 768)
        dx = dx + nt(he[:, :512], w[e, :, :512])
        grads.append(jnp.concatenate([tn(x, he[:, :512]), tn(og, he[:, 512:])], axis=1))
    return dx.astype(BF16), jnp.stack(grads).astype(BF16)


def shards(tokens, out_grad, expert_ids, route_weight, w_gate, w_up, w_down):
    w_cat = jnp.concatenate([w_gate[0], w_up[0], jnp.transpose(w_down[0])], axis=1)
    ids = jnp.zeros((8, 128), jnp.int32).at[:2].set(jnp.transpose(expert_ids))
    x, og, ids_all, w = spread(tokens, out_grad, ids, w_cat)
    x, og, w = x.reshape(1024, 768), og.reshape(1024, 768), w.reshape(8, 768, 768)
    ids_all = jnp.transpose(ids_all[:, :2], (0, 2, 1)).reshape(1024, 2)
    part = partial_pre(x, og, ids_all, w)
    h = middle(part, jnp.transpose(route_weight).reshape(256, 1))
    dx, grads = backward(x, og, ids_all, w, h)
    d_tokens, g = collect(dx.reshape(8, 128, 768), grads.reshape(8, 2, 384, 768))
    return d_tokens, g[None, :, :256], g[None, :, 256:512], jnp.transpose(g[:, 512:])[None]


def solution(mesh):
    in_specs = (
        P(("dp", "ep"), None),
        P(("dp", "ep"), None),
        P(("dp", "ep"), None),
        P(("dp", "ep"), None),
        P("ep", "dp", None),
        P("ep", "dp", None),
        P("ep", None, "dp"),
    )
    out_specs = (
        P(("dp", "ep"), None),
        P("ep", "dp", None),
        P("ep", "dp", None),
        P("ep", None, "dp"),
    )
    return jax.shard_map(shards, mesh=mesh, in_specs=in_specs, out_specs=out_specs, check_vma=False)
```

```python
import functools

import jax
import jax.numpy as jnp
from jax import lax
from jax.experimental import pallas as pl
from jax.experimental.pallas import tpu as pltpu
from jax.sharding import PartitionSpec as P

MESH = pl.DeviceIdType.MESH
F32, BF16 = jnp.float32, jnp.bfloat16
PEERS = [(dy, dz) for dy in (2, 1, 3, 0) for dz in (1, 0) if (dy, dz) != (0, 0)]


class Spot:
    def __init__(self):
        dp, ep = lax.axis_index("dp"), lax.axis_index("ep")
        self.y, self.zl, self.c = dp // 4, (dp // 2) % 2, dp % 2
        self.zh, self.x = ep // 4, ep % 4
        self.q = dp // 2

    def to(self, y=0, zl=0, c=0, zh=0, x=0):
        dp = (self.y + y) % 4 * 4 + (self.zl + zl) % 2 * 2 + (self.c + c) % 2
        return (dp, (self.zh + zh) % 2 * 4 + (self.x + x) % 4)

    def block(self, y, zl):
        return (self.y + y) % 4 * 2 + (self.zl + zl) % 2

    def expert(self, x, zh):
        return (self.zh + zh) % 2 * 4 + (self.x + x) % 4


class Links:
    def __init__(self, send_sem, recv_sem):
        self.send_sem, self.recv_sem, self.count, self.sent = send_sem, recv_sem, 0, []

    def send(self, src, dst, device):
        n = self.count
        self.count += 1
        copy = pltpu.make_async_remote_copy(
            src_ref=src,
            dst_ref=dst,
            send_sem=self.send_sem.at[n],
            recv_sem=self.recv_sem.at[n],
            device_id=device,
            device_id_type=MESH,
        )
        copy.start()
        self.sent.append(copy)
        return copy

    def finish(self):
        for copy in self.sent:
            copy.wait_send()


def greet(devices):
    barrier = pltpu.get_barrier_semaphore()
    for device in devices:
        pl.semaphore_signal(barrier, inc=1, device_id=device, device_id_type=MESH)
    pl.semaphore_wait(barrier, len(devices))


def add_rows(dst, sources, rows, step=32):
    @pl.loop(0, rows // step)
    def _(i):
        at = pl.ds(pl.multiple_of(i * step, step), step)
        total = sources[0][at, :].astype(F32)
        for source in sources[1:]:
            total = total + source[at, :].astype(F32)
        dst[at, :] = total.astype(dst.dtype)


SPREAD_COPIES = 21 + 1 + 2 + 1 + 3 + 6 + 6 + 4


def spread_kernel(tok, og, ids, w_in, x_out, og_out, ids_out, w_out, send_sem, recv_sem, own_sem):
    me = Spot()
    right, left, core, far = me.to(x=1), me.to(x=3), me.to(c=1), me.to(zh=1)
    greet([me.to(y=dy, zl=dz) for dy, dz in PEERS] + [right, left, core, far])
    links = Links(send_sem, recv_sem)
    own, far_e = me.expert(0, 0), me.expert(0, 1)

    from_far = links.send(w_in, w_out.at[own, me.c], far)
    from_left0 = links.send(w_in, w_out.at[own, me.c], right)
    from_right0 = links.send(w_in, w_out.at[own, me.c], left)
    columns = []
    for dy, dz in PEERS:
        there, device = me.block(dy, dz), me.to(y=dy, zl=dz)
        cols = pl.ds(pl.multiple_of(there * 768, 768), 768)
        columns.append(links.send(tok.at[:, cols], x_out.at[me.q], device))
        columns.append(links.send(og.at[:, cols], og_out.at[me.q], device))
        columns.append(links.send(ids, ids_out.at[me.q], device))
    from_core = [links.send(w_in, w_out.at[own, me.c], core)]
    cols = pl.ds(pl.multiple_of(me.q * 768, 768), 768)
    local = [
        pltpu.make_async_copy(w_in, w_out.at[own, me.c], own_sem.at[0]),
        pltpu.make_async_copy(tok.at[:, cols], x_out.at[me.q], own_sem.at[1]),
        pltpu.make_async_copy(og.at[:, cols], og_out.at[me.q], own_sem.at[2]),
        pltpu.make_async_copy(ids, ids_out.at[me.q], own_sem.at[3]),
    ]
    for copy in local:
        copy.start()

    def pass_on(expert, device, rows=pl.ds(0, 384)):
        piece = w_out.at[expert, me.c, rows, :]
        return links.send(piece, piece, device)

    low, high = pl.ds(0, 192), pl.ds(192, 192)
    from_far.wait_recv()
    from_left1 = pass_on(far_e, right)
    from_right1 = pass_on(far_e, left)
    from_core.append(pass_on(far_e, core))
    halves = []
    for dz, from_left, from_right in ((0, from_left0, from_right0), (1, from_left1, from_right1)):
        from_left.wait_recv()
        halves.append(pass_on(me.expert(3, dz), right, low))
        from_core.append(pass_on(me.expert(3, dz), core))
        from_right.wait_recv()
        halves.append(pass_on(me.expert(1, dz), left, high))
        from_core.append(pass_on(me.expert(1, dz), core))
    for n, half in enumerate(halves):
        half.wait_recv()
        from_core.append(pass_on(me.expert(2, n // 2), core, (low, high)[n % 2]))
    for copy in columns + from_core:
        copy.wait_recv()
    for copy in local:
        copy.wait()
    links.finish()


def spread(tokens, out_grad, ids, w_cat):
    vmem, anywhere = pl.BlockSpec(memory_space=pltpu.VMEM), pl.BlockSpec(memory_space=pl.ANY)
    return pl.pallas_call(
        spread_kernel,
        out_shape=(
            jax.ShapeDtypeStruct((8, 128, 768), BF16),
            jax.ShapeDtypeStruct((8, 128, 768), BF16),
            jax.ShapeDtypeStruct((8, 8, 128), jnp.int32),
            jax.ShapeDtypeStruct((8, 2, 384, 768), BF16),
        ),
        in_specs=[vmem] * 4,
        out_specs=(anywhere,) * 4,
        scratch_shapes=[
            pltpu.SemaphoreType.DMA((SPREAD_COPIES,)),
            pltpu.SemaphoreType.DMA((SPREAD_COPIES,)),
            pltpu.SemaphoreType.DMA((4,)),
        ],
        compiler_params=pltpu.CompilerParams(collective_id=0, has_side_effects=True),
        name="spread",
    )(tokens, out_grad, ids, w_cat)


def activation(pre, weight):
    gate, up, grad_hidden = pre[:, :256], pre[:, 256:512], pre[:, 512:] * weight
    sig = jax.nn.sigmoid(gate)
    silu = gate * sig
    hidden = silu * up * weight
    grad_gate = grad_hidden * up * sig * (1.0 + gate * (1.0 - sig))
    grad_up = grad_hidden * silu
    return grad_gate.astype(BF16), grad_up.astype(BF16), hidden.astype(BF16)


MIDDLE_COPIES = 8 + 4 + 1 + 3 + 2 + 4


def middle_kernel(part, weight, h_out, ra, rb, sa, sb, fl, fr, zs, zr, own, send_sem, recv_sem, own_sem):
    me = Spot()
    right, left, pair = me.to(y=1), me.to(y=3), me.to(zl=1)
    greet([right, left, pair])
    links = Links(send_sem, recv_sem)
    low, high = pl.ds(0, 128), pl.ds(128, 128)

    first_a, first_b, other_b, other_a, last_a, last_b = {}, {}, {}, {}, {}, {}
    for dz in (1, 0):
        first_a[dz] = links.send(part.at[me.block(2, dz), low, :], ra.at[dz], right)
        first_b[dz] = links.send(part.at[me.block(2, dz), high, :], rb.at[dz], left)
    for dz in (1, 0):
        other_b[dz] = links.send(part.at[me.block(1, dz), high, :], fl.at[dz, high, :], right)
        other_a[dz] = links.send(part.at[me.block(3, dz), low, :], fr.at[dz, low, :], left)
    for dz in (1, 0):
        first_a[dz].wait_recv()
        add_rows(sa.at[dz], [part.at[me.block(1, dz), low, :], ra.at[dz]], 128)
        last_a[dz] = links.send(sa.at[dz], fl.at[dz, low, :], right)
        first_b[dz].wait_recv()
        add_rows(sb.at[dz], [part.at[me.block(3, dz), high, :], rb.at[dz]], 128)
        last_b[dz] = links.send(sb.at[dz], fr.at[dz, high, :], left)
    for group in (other_b, other_a, last_a, last_b):
        group[1].wait_recv()
    add_rows(zs, [part.at[me.block(0, 1)], fl.at[1], fr.at[1]], 256)
    cross = links.send(zs, zr, pair)
    for group in (other_b, other_a, last_a, last_b):
        group[0].wait_recv()
    cross.wait_recv()

    @pl.loop(0, 16)
    def _(i):
        at = pl.ds(pl.multiple_of(i * 16, 16), 16)
        pre = part[me.block(0, 0), at, :].astype(F32) + zr[at, :].astype(F32)
        pre = pre + fl[0, at, :].astype(F32) + fr[0, at, :].astype(F32)
        own[at, :256], own[at, 256:512], own[at, 512:] = activation(pre, weight[at, :])

    mine = pltpu.make_async_copy(own, h_out.at[me.q], own_sem)
    mine.start()
    from_pair = links.send(own, h_out.at[me.q], pair)
    from_left0 = links.send(own, h_out.at[me.q], right)
    from_right0 = links.send(own, h_out.at[me.q], left)

    def pass_on(block, device, rows=pl.ds(0, 256)):
        piece = h_out.at[block, rows, :]
        return links.send(piece, piece, device)

    from_pair.wait_recv()
    from_left1 = pass_on(me.block(0, 1), right)
    from_right1 = pass_on(me.block(0, 1), left)
    halves = []
    for dz, from_left, from_right in ((0, from_left0, from_right0), (1, from_left1, from_right1)):
        from_left.wait_recv()
        halves.append(pass_on(me.block(3, dz), right, low))
        from_right.wait_recv()
        halves.append(pass_on(me.block(1, dz), left, high))
    for half in halves:
        half.wait_recv()
    mine.wait()
    links.finish()


def middle(part, weight):
    vmem, anywhere = pl.BlockSpec(memory_space=pltpu.VMEM), pl.BlockSpec(memory_space=pl.ANY)
    half, full = pltpu.VMEM((2, 128, 768), BF16), pltpu.VMEM((2, 256, 768), BF16)
    one = pltpu.VMEM((256, 768), BF16)
    return pl.pallas_call(
        middle_kernel,
        out_shape=jax.ShapeDtypeStruct((8, 256, 768), BF16),
        in_specs=[vmem] * 2,
        out_specs=anywhere,
        scratch_shapes=[half] * 4 + [full] * 2 + [one] * 3 + [
            pltpu.SemaphoreType.DMA((MIDDLE_COPIES,)),
            pltpu.SemaphoreType.DMA((MIDDLE_COPIES,)),
            pltpu.SemaphoreType.DMA,
        ],
        compiler_params=pltpu.CompilerParams(collective_id=1, has_side_effects=True),
        name="middle",
    )(part, weight)


FINISH_COPIES = 7 + 8 + 4 + 4 + 4 + 1
ORDER = ((2, 1), (1, 1), (3, 1), (2, 0), (1, 0), (3, 0), (0, 1), (0, 0))


def finish_kernel(
    x, og, ids, h, w, d_out, g_out,
    xt, ogt, w_all, he, g, cr, dx, a2, ra, rb, sa, sb, oa, ob, fl, fr, zs, zr,
    send_sem, recv_sem, w_sem, own_sem,
):
    me = Spot()
    right, left, core, far = me.to(x=1), me.to(x=3), me.to(c=1), me.to(zh=1)
    loads = [pltpu.make_async_copy(w.at[e], w_all.at[e], w_sem.at[e]) for e in range(8)]
    for load in loads:
        load.start()
    for q in range(8):
        xt[:, q * 128 : q * 128 + 128] = jnp.transpose(x[q])
        ogt[:, q * 128 : q * 128 + 128] = jnp.transpose(og[q])
    greet([me.to(y=dy, zl=dz) for dy, dz in PEERS] + [right, left, core, far])
    links = Links(send_sem, recv_sem)
    low, high = pl.ds(0, 192), pl.ds(192, 192)
    mine, others = me.c, 1 - me.c
    swapped, first_a, first_b, other_b, other_a, last_a, last_b = {}, {}, {}, {}, {}, {}, {}

    def product(step, dz):
        e = me.expert(step, dz)

        @pl.loop(0, 32)
        def _(i):
            at = pl.ds(pl.multiple_of(i * 32, 32), 32)
            q, row = i // 4, pl.multiple_of(i % 4 * 32, 32)
            m0 = (ids[at, 0:1] == e).astype(F32)
            m1 = (ids[at, 1:2] == e).astype(F32)
            h0 = h[q, pl.ds(row, 32), :].astype(F32)
            h1 = h[q, pl.ds(row + 128, 32), :].astype(F32)
            he[e, at, :] = (h0 * m0 + h1 * m1).astype(BF16)

        for n, left_t in ((0, xt), (1, xt), (2, ogt)):
            cols = slice(n * 256, n * 256 + 256)
            out = jnp.dot(left_t[...], he[e, :, cols], preferred_element_type=F32).astype(BF16)
            g[e, 0, :, cols] = out[:384]
            g[e, 1, :, cols] = out[384:]
        swapped[step, dz] = links.send(g.at[e, others], cr.at[e], core)

    def start_far(dz):
        e = me.expert(2, dz)
        swapped[2, dz].wait_recv()
        add_rows(a2.at[dz], [g.at[e, mine], cr.at[e]], 384)
        first_a[dz] = links.send(a2.at[dz, low, :], ra.at[dz], right)
        first_b[dz] = links.send(a2.at[dz, high, :], rb.at[dz], left)

    def start_near(dz):
        e = me.expert(1, dz)
        swapped[1, dz].wait_recv()
        add_rows(ob.at[dz], [g.at[e, mine, high, :], cr.at[e, high, :]], 192)
        other_b[dz] = links.send(ob.at[dz], fl.at[dz, high, :], right)
        e = me.expert(3, dz)
        swapped[3, dz].wait_recv()
        add_rows(oa.at[dz], [g.at[e, mine, low, :], cr.at[e, low, :]], 192)
        other_a[dz] = links.send(oa.at[dz], fr.at[dz, low, :], left)

    def relay(dz):
        e = me.expert(1, dz)
        first_a[dz].wait_recv()
        add_rows(sa.at[dz], [g.at[e, mine, low, :], cr.at[e, low, :], ra.at[dz]], 192)
        last_a[dz] = links.send(sa.at[dz], fl.at[dz, low, :], right)
        e = me.expert(3, dz)
        first_b[dz].wait_recv()
        add_rows(sb.at[dz], [g.at[e, mine, high, :], cr.at[e, high, :], rb.at[dz]], 192)
        last_b[dz] = links.send(sb.at[dz], fr.at[dz, high, :], left)

    def token_part(n):
        cols = slice(n * 256, n * 256 + 256)
        total = None
        for e in range(8):
            part = lax.dot_general(
                he[e, :, :512], w_all[e, cols, :512], (((1,), (1,)), ((), ())), preferred_element_type=F32
            )
            total = part if total is None else total + part
        for q in range(8):
            dx[q, :, cols] = total[q * 128 : q * 128 + 128].astype(BF16)

    product(2, 1)
    product(1, 1)
    start_far(1)
    product(3, 1)
    product(2, 0)
    start_near(1)
    product(1, 0)
    start_far(0)
    product(3, 0)
    product(0, 1)
    start_near(0)
    relay(1)
    product(0, 0)
    for load in loads:
        load.wait()
    token_part(0)
    token_part(1)
    token_part(2)
    back = []
    cols = pl.ds(pl.multiple_of(me.q * 768, 768), 768)
    for dy, dz in PEERS:
        back.append(links.send(dx.at[me.block(dy, dz)], d_out.at[:, cols], me.to(y=dy, zl=dz)))
    keep = pltpu.make_async_copy(dx.at[me.q], d_out.at[:, cols], own_sem)
    keep.start()
    relay(0)
    for group in (other_b, other_a, last_a, last_b):
        group[1].wait_recv()
    e = me.expert(0, 1)
    swapped[0, 1].wait_recv()
    add_rows(zs, [g.at[e, mine], cr.at[e], fl.at[1], fr.at[1]], 384)
    cross = links.send(zs, zr, far)
    for group in (other_b, other_a, last_a, last_b):
        group[0].wait_recv()
    swapped[0, 0].wait_recv()
    cross.wait_recv()
    e = me.expert(0, 0)
    add_rows(g_out, [g.at[e, mine], cr.at[e], fl.at[0], fr.at[0], zr], 384)
    for copy in back:
        copy.wait_recv()
    keep.wait()
    links.finish()


def finish(x, og, ids, h, w):
    vmem, anywhere = pl.BlockSpec(memory_space=pltpu.VMEM), pl.BlockSpec(memory_space=pl.ANY)
    half, full = pltpu.VMEM((2, 192, 768), BF16), pltpu.VMEM((2, 384, 768), BF16)
    one = pltpu.VMEM((384, 768), BF16)
    return pl.pallas_call(
        finish_kernel,
        out_shape=(
            jax.ShapeDtypeStruct((128, 6144), BF16),
            jax.ShapeDtypeStruct((384, 768), F32),
        ),
        in_specs=[vmem] * 4 + [anywhere],
        out_specs=(anywhere, vmem),
        scratch_shapes=[
            pltpu.VMEM((768, 1024), BF16),
            pltpu.VMEM((768, 1024), BF16),
            pltpu.VMEM((8, 768, 768), BF16),
            pltpu.VMEM((8, 1024, 768), BF16),
            pltpu.VMEM((8, 2, 384, 768), BF16),
            pltpu.VMEM((8, 384, 768), BF16),
            pltpu.VMEM((8, 128, 768), BF16),
        ]
        + [full] + [half] * 6 + [full] * 2 + [one] * 2
        + [
            pltpu.SemaphoreType.DMA((FINISH_COPIES,)),
            pltpu.SemaphoreType.DMA((FINISH_COPIES,)),
            pltpu.SemaphoreType.DMA((8,)),
            pltpu.SemaphoreType.DMA,
        ],
        compiler_params=pltpu.CompilerParams(collective_id=2, has_side_effects=True, vmem_limit_bytes=60 << 20),
        name="finish",
    )(x, og, ids, h, w)


def partial_pre(x, og, ids_all, w):
    total = [jnp.zeros((1024, 768), F32) for _ in range(2)]
    for e in range(8):
        y = jnp.concatenate(
            [
                jnp.dot(x, w[e, :, :512], preferred_element_type=F32),
                jnp.dot(og, w[e, :, 512:], preferred_element_type=F32),
            ],
            axis=1,
        )
        for k in range(2):
            total[k] = jnp.where(ids_all[:, k : k + 1] == e, y, total[k])
    both = jnp.stack([t.reshape(8, 128, 768) for t in total], axis=1)
    return both.reshape(8, 256, 768).astype(BF16)


def shards(tokens, out_grad, expert_ids, route_weight, w_gate, w_up, w_down):
    w_cat = jnp.concatenate([w_gate[0], w_up[0], jnp.transpose(w_down[0])], axis=1)
    ids = jnp.zeros((8, 128), jnp.int32).at[:2].set(jnp.transpose(expert_ids))
    x, og, ids_all, w = spread(tokens, out_grad, ids, w_cat)
    w = w.reshape(8, 768, 768)
    ids_all = jnp.transpose(ids_all[:, :2], (0, 2, 1)).reshape(1024, 2)
    part = partial_pre(x.reshape(1024, 768), og.reshape(1024, 768), ids_all, w)
    h = middle(part, jnp.transpose(route_weight).reshape(256, 1))
    d_tokens, g = finish(x, og, ids_all, h, w)
    return d_tokens, g[None, :, :256], g[None, :, 256:512], jnp.transpose(g[:, 512:])[None]


def solution(mesh):
    in_specs = (
        P(("dp", "ep"), None),
        P(("dp", "ep"), None),
        P(("dp", "ep"), None),
        P(("dp", "ep"), None),
        P("ep", "dp", None),
        P("ep", "dp", None),
        P("ep", None, "dp"),
    )
    out_specs = (
        P(("dp", "ep"), None),
        P("ep", "dp", None),
        P("ep", "dp", None),
        P("ep", None, "dp"),
    )
    return jax.shard_map(shards, mesh=mesh, in_specs=in_specs, out_specs=out_specs, check_vma=False)
```

```python
import functools

import jax
import jax.numpy as jnp
from jax import lax
from jax.experimental import pallas as pl
from jax.experimental.pallas import tpu as pltpu
from jax.sharding import PartitionSpec as P

MESH = pl.DeviceIdType.MESH
F32, BF16 = jnp.float32, jnp.bfloat16
PEERS = [(dy, dz) for dy in (2, 1, 3, 0) for dz in (1, 0) if (dy, dz) != (0, 0)]


class Spot:
    def __init__(self):
        dp, ep = lax.axis_index("dp"), lax.axis_index("ep")
        self.y, self.zl, self.c = dp // 4, (dp // 2) % 2, dp % 2
        self.zh, self.x = ep // 4, ep % 4
        self.b = self.block(0, 0)

    def to(self, y=0, zl=0, c=0, zh=0, x=0):
        dp = (self.y + y) % 4 * 4 + (self.zl + zl) % 2 * 2 + (self.c + c) % 2
        return (dp, (self.zh + zh) % 2 * 4 + (self.x + x) % 4)

    def block(self, y, zl):
        return (self.zl + zl) % 2 * 4 + (self.y + y) % 4

    def columns(self, y, zl, width=768, offset=0):
        start = ((self.y + y) % 4 * 2 + (self.zl + zl) % 2) * 768 + offset
        return pl.ds(pl.multiple_of(start, 128), width)

    def expert(self, x, zh):
        return (self.zh + zh) % 2 * 4 + (self.x + x) % 4


class Links:
    def __init__(self, send_sem, recv_sem):
        self.send_sem, self.recv_sem, self.count, self.sent = send_sem, recv_sem, 0, []

    def send(self, src, dst, device):
        n = self.count
        self.count += 1
        copy = pltpu.make_async_remote_copy(
            src_ref=src,
            dst_ref=dst,
            send_sem=self.send_sem.at[n],
            recv_sem=self.recv_sem.at[n],
            device_id=device,
            device_id_type=MESH,
        )
        copy.start()
        self.sent.append(copy)
        return copy

    def finish(self):
        assert self.count == self.send_sem.shape[0]
        for copy in self.sent:
            copy.wait_send()


def greet(devices):
    barrier = pltpu.get_barrier_semaphore()
    for device in devices:
        pl.semaphore_signal(barrier, inc=1, device_id=device, device_id_type=MESH)
    pl.semaphore_wait(barrier, len(devices))


def add_rows(dst, sources, rows, step=32):
    @pl.loop(0, rows // step)
    def _(i):
        at = pl.ds(pl.multiple_of(i * step, step), step)
        total = sources[0][at, :].astype(F32)
        for source in sources[1:]:
            total = total + source[at, :].astype(F32)
        dst[at, :] = total.astype(dst.dtype)


SPREAD_COPIES = 19 + 24 + 7


def spread_kernel(
    tok, og, ids, w_in, part, xt, ogt, idc, w_out,
    x, g, ids_in, w, z_tok, z_og, l_tok, r_og, send_sem, recv_sem, own_sem, w_sem,
):
    me = Spot()
    right, left, up, down = me.to(x=1), me.to(x=3), me.to(y=1), me.to(y=3)
    core, far, pair = me.to(c=1), me.to(zh=1), me.to(zl=1)
    greet([me.to(y=dy, zl=dz) for dy, dz in PEERS] + [right, left, core, far])
    links = Links(send_sem, recv_sem)
    own, far_e = me.expert(0, 0), me.expert(0, 1)

    from_far = links.send(w_in, w.at[own, me.c], far)
    from_left0 = links.send(w_in, w.at[own, me.c], right)
    from_right0 = links.send(w_in, w.at[own, me.c], left)
    from_core = {(0, 0): [links.send(w_in, w.at[own, me.c], core)]}

    def cut(array, y, zl):
        return array.at[:, me.columns(y, zl)]

    plane = [
        links.send(cut(tok, 2, 0), l_tok.at[0], up),
        links.send(cut(og, 2, 0), r_og.at[0], down),
    ]
    z_in = {}
    z_in[2, 0] = links.send(cut(tok, 2, 1), z_tok.at[2], pair)
    z_in[2, 1] = links.send(cut(og, 2, 1), z_og.at[2], pair)
    near = []
    for y, device in ((1, up), (3, down)):
        near.append(links.send(cut(tok, y, 0), x.at[me.b], device))
        near.append(links.send(cut(og, y, 0), g.at[me.b], device))
    for y in (1, 3):
        z_in[y, 0] = links.send(cut(tok, y, 1), z_tok.at[y], pair)
        z_in[y, 1] = links.send(cut(og, y, 1), z_og.at[y], pair)
    z_in[0, 0] = links.send(cut(tok, 0, 1), x.at[me.b], pair)
    z_in[0, 1] = links.send(cut(og, 0, 1), g.at[me.b], pair)
    names = [links.send(ids, ids_in.at[me.b], me.to(y=dy, zl=dz)) for dy, dz in PEERS]
    local = [
        pltpu.make_async_copy(w_in, w.at[own, me.c], own_sem.at[0]),
        pltpu.make_async_copy(cut(tok, 0, 0), x.at[me.b], own_sem.at[1]),
        pltpu.make_async_copy(cut(og, 0, 0), g.at[me.b], own_sem.at[2]),
        pltpu.make_async_copy(ids, ids_in.at[me.b], own_sem.at[3]),
    ]
    for copy in local:
        copy.start()

    @pl.loop(0, 64)
    def _(i):
        part[i // 8, pl.ds(pl.multiple_of(i % 8 * 32, 32), 32), :] = jnp.zeros((32, 768), BF16)

    def pass_on(expert, device, rows=pl.ds(0, 384)):
        piece = w.at[expert, me.c, rows, :]
        return links.send(piece, piece, device)

    low, high = pl.ds(0, 192), pl.ds(192, 192)
    across, ends = [], []
    z_in[2, 0].wait_recv()
    across.append(links.send(z_tok.at[2], l_tok.at[1], up))
    plane[0].wait_recv()
    ends.append(links.send(l_tok.at[0], x.at[me.block(3, 0)], up))
    z_in[2, 1].wait_recv()
    across.append(links.send(z_og.at[2], r_og.at[1], down))
    plane[1].wait_recv()
    ends.append(links.send(r_og.at[0], g.at[me.block(1, 0)], down))
    halves = {0: [], 1: []}

    def sideways(dz, from_left, from_right):
        from_left.wait_recv()
        halves[dz].append(pass_on(me.expert(3, dz), right, low))
        from_core[3, dz] = [pass_on(me.expert(3, dz), core)]
        from_right.wait_recv()
        halves[dz].append(pass_on(me.expert(1, dz), left, high))
        from_core[1, dz] = [pass_on(me.expert(1, dz), core)]

    sideways(0, from_left0, from_right0)
    late = []

    def partner(y, device):
        z_in[y, 0].wait_recv()
        late.append(links.send(z_tok.at[y], x.at[me.block(0, 1)], device))
        z_in[y, 1].wait_recv()
        late.append(links.send(z_og.at[y], g.at[me.block(0, 1)], device))

    partner(1, up)
    from_far.wait_recv()
    from_left1 = pass_on(far_e, right)
    from_right1 = pass_on(far_e, left)
    from_core[0, 1] = [pass_on(far_e, core)]
    partner(3, down)
    across[0].wait_recv()
    late.append(links.send(l_tok.at[1], x.at[me.block(3, 1)], up))
    across[1].wait_recv()
    late.append(links.send(r_og.at[1], g.at[me.block(1, 1)], down))

    def second(dz):
        from_core[2, dz] = []
        for n, half in enumerate(halves[dz]):
            half.wait_recv()
            from_core[2, dz].append(pass_on(me.expert(2, dz), core, (low, high)[n]))

    def turn(dz):
        for y in range(4):
            b = me.block(y, dz)
            at = pl.ds(pl.multiple_of(b * 128, 128), 128)
            xt[:, at] = jnp.transpose(x[b])
            ogt[:, at] = jnp.transpose(g[b])
            idc[at, :] = jnp.transpose(ids_in[b])

    def keep(step, dz):
        for copy in from_core[step, dz]:
            copy.wait_recv()
        e = me.expert(step, dz)
        pltpu.make_async_copy(w.at[e], w_out.at[e], w_sem.at[e]).start()

    def product(e, dz):
        plane_at = pl.multiple_of((me.zl + dz) % 2 * 4, 4)
        for n, source in ((0, x), (1, x), (2, g)):
            cols = slice(n * 256, n * 256 + 256)
            rows = source[pl.ds(plane_at, 4)].reshape(512, 768)
            out = jnp.dot(rows, w[e, :, :, cols].reshape(768, 256), preferred_element_type=F32)
            for y in range(4):
                names_at = pl.ds(pl.multiple_of((plane_at + y) * 128, 128), 128)
                for k in range(2):
                    here = part.at[plane_at + y, k * 128 : k * 128 + 128, cols]
                    chosen = idc[names_at, k : k + 1] == e
                    old = here[...].astype(F32)
                    here[...] = jnp.where(chosen, out[y * 128 : y * 128 + 128], old).astype(BF16)

    def first_six(i):
        g2 = i // 2
        step = (g2 + 1) // 2 * (1 + 2 * (i % 2))
        return me.expert(step, (1 - (g2 + 1) // 2) * (i % 2) + g2 // 2)

    for copy in near + ends + names:
        copy.wait_recv()
    for copy in local:
        copy.wait()
    turn(0)
    for step, dz in ((0, 0), (0, 1), (1, 0), (3, 0)):
        keep(step, dz)

    @pl.loop(0, 4)
    def _(i):
        product(first_six(i), 0)

    second(0)
    sideways(1, from_left1, from_right1)
    keep(1, 1)
    keep(3, 1)

    @pl.loop(4, 6)
    def _(i):
        product(first_six(i), 0)

    second(1)
    for copy in [z_in[0, 0], z_in[0, 1]] + late:
        copy.wait_recv()
    turn(1)

    @pl.loop(0, 6)
    def _(i):
        product(first_six(i), 1)

    keep(2, 0)
    keep(2, 1)

    @pl.loop(0, 4)
    def _(i):
        product(me.expert(2, i % 2), i // 2)

    links.finish()
    for e in range(8):
        pltpu.make_async_copy(w.at[e], w_out.at[e], w_sem.at[e]).wait()


def spread(tokens, out_grad, ids, w_cat):
    vmem, anywhere = pl.BlockSpec(memory_space=pltpu.VMEM), pl.BlockSpec(memory_space=pl.ANY)
    blocks = lambda n: pltpu.VMEM((n, 128, 768), BF16)
    return pl.pallas_call(
        spread_kernel,
        out_shape=(
            jax.ShapeDtypeStruct((8, 256, 768), BF16),
            jax.ShapeDtypeStruct((768, 1024), BF16),
            jax.ShapeDtypeStruct((768, 1024), BF16),
            jax.ShapeDtypeStruct((1024, 8), jnp.int32),
            jax.ShapeDtypeStruct((8, 2, 384, 768), BF16),
        ),
        in_specs=[vmem] * 4,
        out_specs=(vmem,) * 4 + (anywhere,),
        scratch_shapes=[
            blocks(8),
            blocks(8),
            pltpu.VMEM((8, 8, 128), jnp.int32),
            pltpu.VMEM((8, 2, 384, 768), BF16),
            blocks(4),
            blocks(4),
            blocks(2),
            blocks(2),
            pltpu.SemaphoreType.DMA((SPREAD_COPIES,)),
            pltpu.SemaphoreType.DMA((SPREAD_COPIES,)),
            pltpu.SemaphoreType.DMA((4,)),
            pltpu.SemaphoreType.DMA((8,)),
        ],
        compiler_params=pltpu.CompilerParams(collective_id=0, has_side_effects=True, vmem_limit_bytes=60 << 20),
        name="spread",
    )(tokens, out_grad, ids, w_cat)


def activation(pre, weight):
    gate, up, grad_hidden = pre[:, :256], pre[:, 256:512], pre[:, 512:] * weight
    sig = jax.nn.sigmoid(gate)
    silu = gate * sig
    hidden = silu * up * weight
    grad_gate = grad_hidden * up * sig * (1.0 + gate * (1.0 - sig))
    grad_up = grad_hidden * silu
    return grad_gate.astype(BF16), grad_up.astype(BF16), hidden.astype(BF16)


MIDDLE_COPIES = 13 + 10 + 9 + 8


def middle_kernel(
    part, weight, h_out, ra, rb, sa, sb, fl, fr, zs, zr, zin, s2, s1, s3, ra2, rb2, sa2, sb2, fl2, fr2, own,
    send_sem, recv_sem, own_sem,
):
    me = Spot()
    right, left, pair = me.to(y=1), me.to(y=3), me.to(zl=1)
    greet([right, left, pair])
    links = Links(send_sem, recv_sem)
    low, high = pl.ds(0, 64), pl.ds(64, 64)
    k0, k1, k1_low, k1_high = pl.ds(0, 128), pl.ds(128, 128), pl.ds(128, 64), pl.ds(192, 64)

    first_a, first_b, other_b, other_a, last_a, last_b, z_in = {}, {}, {}, {}, {}, {}, {}
    z_in[2] = links.send(part.at[me.block(2, 1), k1, :], zin.at[2], pair)
    for dz in (1, 0):
        first_a[dz] = links.send(part.at[me.block(2, dz), low, :], ra.at[dz], right)
        first_b[dz] = links.send(part.at[me.block(2, dz), high, :], rb.at[dz], left)
    for y in (1, 3, 0):
        z_in[y] = links.send(part.at[me.block(y, 1), k1, :], zin.at[y], pair)
    for dz in (1, 0):
        other_b[dz] = links.send(part.at[me.block(1, dz), high, :], fl.at[dz, high, :], right)
        other_a[dz] = links.send(part.at[me.block(3, dz), low, :], fr.at[dz, low, :], left)

    def relay(dz):
        first_a[dz].wait_recv()
        add_rows(sa.at[dz], [part.at[me.block(1, dz), low, :], ra.at[dz]], 64)
        last_a[dz] = links.send(sa.at[dz], fl.at[dz, low, :], right)
        first_b[dz].wait_recv()
        add_rows(sb.at[dz], [part.at[me.block(3, dz), high, :], rb.at[dz]], 64)
        last_b[dz] = links.send(sb.at[dz], fr.at[dz, high, :], left)

    relay(1)
    z_in[2].wait_recv()
    add_rows(s2, [part.at[me.block(2, 0), k1, :], zin.at[2]], 128)
    far_a = links.send(s2.at[low, :], ra2, right)
    far_b = links.send(s2.at[high, :], rb2, left)
    relay(0)
    z_in[1].wait_recv()
    add_rows(s1, [part.at[me.block(1, 0), k1_high, :], zin.at[1, high, :]], 64)
    side_b = links.send(s1, fl2.at[high, :], right)
    for group in (other_b, other_a, last_a, last_b):
        group[1].wait_recv()
    add_rows(zs, [part.at[me.block(0, 1), k0, :], fl.at[1], fr.at[1]], 128)
    cross = links.send(zs, zr, pair)
    z_in[3].wait_recv()
    add_rows(s3, [part.at[me.block(3, 0), k1_low, :], zin.at[3, low, :]], 64)
    side_a = links.send(s3, fr2.at[low, :], left)
    far_a.wait_recv()
    add_rows(sa2, [part.at[me.block(1, 0), k1_low, :], zin.at[1, low, :], ra2], 64)
    end_a = links.send(sa2, fl2.at[low, :], right)
    far_b.wait_recv()
    add_rows(sb2, [part.at[me.block(3, 0), k1_high, :], zin.at[3, high, :], rb2], 64)
    end_b = links.send(sb2, fr2.at[high, :], left)

    def active(start, sources):
        @pl.loop(0, 8)
        def _(i):
            row = pl.multiple_of(i * 16, 16)
            at = pl.ds(start + row, 16)
            pre = part[me.b, at, :].astype(F32)
            for source in sources:
                pre = pre + source[pl.ds(row, 16), :].astype(F32)
            own[at, :256], own[at, 256:512], own[at, 512:] = activation(pre, weight[at, :])

    for group in (other_b, other_a, last_a, last_b):
        group[0].wait_recv()
    cross.wait_recv()
    active(0, [fl.at[0], fr.at[0], zr])
    mine0 = pltpu.make_async_copy(own.at[k0, :], h_out.at[me.b, k0, :], own_sem.at[0])
    mine0.start()
    from_pair = links.send(own.at[k0, :], h_out.at[me.b, k0, :], pair)
    from_left = {0: links.send(own.at[k0, :], h_out.at[me.b, k0, :], right)}
    from_right = {0: links.send(own.at[k0, :], h_out.at[me.b, k0, :], left)}

    def pass_on(block, device, rows):
        piece = h_out.at[block, rows, :]
        return links.send(piece, piece, device)

    for copy in (z_in[0], side_a, side_b, end_a, end_b):
        copy.wait_recv()
    active(128, [zin.at[0], fl2, fr2])
    mine1 = pltpu.make_async_copy(own.at[k1, :], h_out.at[me.b, k1, :], own_sem.at[1])
    mine1.start()
    left1 = links.send(own.at[k1, :], h_out.at[me.b, k1, :], right)
    right1 = links.send(own.at[k1, :], h_out.at[me.b, k1, :], left)
    tail = [links.send(own.at[k1, :], h_out.at[me.b, k1, :], pair)]
    from_pair.wait_recv()
    from_left[1] = pass_on(me.block(0, 1), right, k0)
    from_right[1] = pass_on(me.block(0, 1), left, k0)
    from_left[0].wait_recv()
    tail.append(pass_on(me.block(3, 0), right, low))
    from_right[0].wait_recv()
    tail.append(pass_on(me.block(1, 0), left, high))
    left1.wait_recv()
    half_a = pass_on(me.block(3, 0), right, k1_low)
    tail.append(pass_on(me.block(3, 0), pair, k1))
    right1.wait_recv()
    half_b = pass_on(me.block(1, 0), left, k1_high)
    tail.append(pass_on(me.block(1, 0), pair, k1))
    from_left[1].wait_recv()
    tail.append(pass_on(me.block(3, 1), right, low))
    from_right[1].wait_recv()
    tail.append(pass_on(me.block(1, 1), left, high))
    half_a.wait_recv()
    half_b.wait_recv()
    tail.append(pass_on(me.block(2, 0), pair, k1))
    for copy in tail:
        copy.wait_recv()
    mine0.wait()
    mine1.wait()
    links.finish()


def middle(part, weight):
    vmem, anywhere = pl.BlockSpec(memory_space=pltpu.VMEM), pl.BlockSpec(memory_space=pl.ANY)
    rows = lambda *shape: pltpu.VMEM(shape + (768,), BF16)
    return pl.pallas_call(
        middle_kernel,
        out_shape=jax.ShapeDtypeStruct((8, 256, 768), BF16),
        in_specs=[vmem] * 2,
        out_specs=anywhere,
        scratch_shapes=[rows(2, 64)] * 4
        + [rows(2, 128)] * 2
        + [rows(128)] * 2
        + [rows(4, 128), rows(128)]
        + [rows(64)] * 6
        + [rows(128)] * 2
        + [
            rows(256),
            pltpu.SemaphoreType.DMA((MIDDLE_COPIES,)),
            pltpu.SemaphoreType.DMA((MIDDLE_COPIES,)),
            pltpu.SemaphoreType.DMA((2,)),
        ],
        compiler_params=pltpu.CompilerParams(collective_id=1, has_side_effects=True),
        name="middle",
    )(part, weight)


FINISH_COPIES = 7 + 8 + 4 + 4 + 4 + 1
ORDER = ((2, 1), (1, 1), (3, 1), (2, 0), (1, 0), (3, 0), (0, 1), (0, 0))


def finish_kernel(
    xt, ogt, ids, h, w, d_out, g_out,
    w_all, he, g, cr, dx, a2, ra, rb, sa, sb, oa, ob, fl, fr, zs, zr,
    send_sem, recv_sem, w_sem, own_sem,
):
    me = Spot()
    right, left, core, far = me.to(x=1), me.to(x=3), me.to(c=1), me.to(zh=1)
    loads = [pltpu.make_async_copy(w.at[e], w_all.at[e], w_sem.at[e]) for e in range(8)]
    for load in loads:
        load.start()
    greet([me.to(y=dy, zl=dz) for dy, dz in PEERS] + [right, left, core, far])
    links = Links(send_sem, recv_sem)
    low, high = pl.ds(0, 192), pl.ds(192, 192)
    mine, others = me.c, 1 - me.c
    swapped, first_a, first_b, other_b, other_a, last_a, last_b = {}, {}, {}, {}, {}, {}, {}

    def product(step, dz):
        e = me.expert(step, dz)

        @pl.loop(0, 32)
        def _(i):
            at = pl.ds(pl.multiple_of(i * 32, 32), 32)
            q, row = i // 4, pl.multiple_of(i % 4 * 32, 32)
            m0 = (ids[at, 0:1] == e).astype(F32)
            m1 = (ids[at, 1:2] == e).astype(F32)
            h0 = h[q, pl.ds(row, 32), :].astype(F32)
            h1 = h[q, pl.ds(row + 128, 32), :].astype(F32)
            he[e, at, :] = (h0 * m0 + h1 * m1).astype(BF16)

        for n, left_t in ((0, xt), (1, xt), (2, ogt)):
            cols = slice(n * 256, n * 256 + 256)
            out = jnp.dot(left_t[...], he[e, :, cols], preferred_element_type=F32).astype(BF16)
            g[e, 0, :, cols] = out[:384]
            g[e, 1, :, cols] = out[384:]
        swapped[step, dz] = links.send(g.at[e, others], cr.at[e], core)

    def start_far(dz):
        e = me.expert(2, dz)
        swapped[2, dz].wait_recv()
        add_rows(a2.at[dz], [g.at[e, mine], cr.at[e]], 384)
        first_a[dz] = links.send(a2.at[dz, low, :], ra.at[dz], right)
        first_b[dz] = links.send(a2.at[dz, high, :], rb.at[dz], left)

    def start_near(dz):
        e = me.expert(1, dz)
        swapped[1, dz].wait_recv()
        add_rows(ob.at[dz], [g.at[e, mine, high, :], cr.at[e, high, :]], 192)
        other_b[dz] = links.send(ob.at[dz], fl.at[dz, high, :], right)
        e = me.expert(3, dz)
        swapped[3, dz].wait_recv()
        add_rows(oa.at[dz], [g.at[e, mine, low, :], cr.at[e, low, :]], 192)
        other_a[dz] = links.send(oa.at[dz], fr.at[dz, low, :], left)

    def relay(dz):
        e = me.expert(1, dz)
        first_a[dz].wait_recv()
        add_rows(sa.at[dz], [g.at[e, mine, low, :], cr.at[e, low, :], ra.at[dz]], 192)
        last_a[dz] = links.send(sa.at[dz], fl.at[dz, low, :], right)
        e = me.expert(3, dz)
        first_b[dz].wait_recv()
        add_rows(sb.at[dz], [g.at[e, mine, high, :], cr.at[e, high, :], rb.at[dz]], 192)
        last_b[dz] = links.send(sb.at[dz], fr.at[dz, high, :], left)

    def token_part(n):
        cols = slice(n * 256, n * 256 + 256)
        total = None
        for e in range(8):
            part = lax.dot_general(
                he[e, :, :512], w_all[e, cols, :512], (((1,), (1,)), ((), ())), preferred_element_type=F32
            )
            total = part if total is None else total + part
        for q in range(8):
            dx[q, :, cols] = total[q * 128 : q * 128 + 128].astype(BF16)

    product(2, 1)
    product(1, 1)
    start_far(1)
    product(3, 1)
    product(2, 0)
    start_near(1)
    product(1, 0)
    start_far(0)
    product(3, 0)
    product(0, 1)
    start_near(0)
    relay(1)
    product(0, 0)
    for load in loads:
        load.wait()
    token_part(0)
    token_part(1)
    token_part(2)
    back = []
    cols = me.columns(0, 0)
    for dy, dz in PEERS:
        back.append(links.send(dx.at[me.block(dy, dz)], d_out.at[:, cols], me.to(y=dy, zl=dz)))
    keep = pltpu.make_async_copy(dx.at[me.b], d_out.at[:, cols], own_sem)
    keep.start()
    relay(0)
    for group in (other_b, other_a, last_a, last_b):
        group[1].wait_recv()
    e = me.expert(0, 1)
    swapped[0, 1].wait_recv()
    add_rows(zs, [g.at[e, mine], cr.at[e], fl.at[1], fr.at[1]], 384)
    cross = links.send(zs, zr, far)
    for group in (other_b, other_a, last_a, last_b):
        group[0].wait_recv()
    swapped[0, 0].wait_recv()
    cross.wait_recv()
    e = me.expert(0, 0)
    add_rows(g_out, [g.at[e, mine], cr.at[e], fl.at[0], fr.at[0], zr], 384)
    for copy in back:
        copy.wait_recv()
    keep.wait()
    links.finish()


def finish(xt, ogt, ids, h, w):
    vmem, anywhere = pl.BlockSpec(memory_space=pltpu.VMEM), pl.BlockSpec(memory_space=pl.ANY)
    half, full = pltpu.VMEM((2, 192, 768), BF16), pltpu.VMEM((2, 384, 768), BF16)
    one = pltpu.VMEM((384, 768), BF16)
    return pl.pallas_call(
        finish_kernel,
        out_shape=(
            jax.ShapeDtypeStruct((128, 6144), BF16),
            jax.ShapeDtypeStruct((384, 768), F32),
        ),
        in_specs=[vmem] * 4 + [anywhere],
        out_specs=(anywhere, vmem),
        scratch_shapes=[
            pltpu.VMEM((8, 768, 768), BF16),
            pltpu.VMEM((8, 1024, 768), BF16),
            pltpu.VMEM((8, 2, 384, 768), BF16),
            pltpu.VMEM((8, 384, 768), BF16),
            pltpu.VMEM((8, 128, 768), BF16),
        ]
        + [full] + [half] * 6 + [full] * 2 + [one] * 2
        + [
            pltpu.SemaphoreType.DMA((FINISH_COPIES,)),
            pltpu.SemaphoreType.DMA((FINISH_COPIES,)),
            pltpu.SemaphoreType.DMA((8,)),
            pltpu.SemaphoreType.DMA,
        ],
        compiler_params=pltpu.CompilerParams(collective_id=2, has_side_effects=True, vmem_limit_bytes=60 << 20),
        name="finish",
    )(xt, ogt, ids, h, w)


def shards(tokens, out_grad, expert_ids, route_weight, w_gate, w_up, w_down):
    w_cat = jnp.concatenate([w_gate[0], w_up[0], jnp.transpose(w_down[0])], axis=1)
    ids = jnp.zeros((8, 128), jnp.int32).at[:2].set(jnp.transpose(expert_ids))
    part, xt, ogt, names, w = spread(tokens, out_grad, ids, w_cat)
    h = middle(part, jnp.transpose(route_weight).reshape(256, 1))
    d_tokens, g = finish(xt, ogt, names, h, w.reshape(8, 768, 768))
    return d_tokens, g[None, :, :256], g[None, :, 256:512], jnp.transpose(g[:, 512:])[None]


def solution(mesh):
    in_specs = (
        P(("dp", "ep"), None),
        P(("dp", "ep"), None),
        P(("dp", "ep"), None),
        P(("dp", "ep"), None),
        P("ep", "dp", None),
        P("ep", "dp", None),
        P("ep", None, "dp"),
    )
    out_specs = (
        P(("dp", "ep"), None),
        P("ep", "dp", None),
        P("ep", "dp", None),
        P("ep", None, "dp"),
    )
    return jax.shard_map(shards, mesh=mesh, in_specs=in_specs, out_specs=out_specs, check_vma=False)
```

```python
import functools

import jax
import jax.numpy as jnp
from jax import lax
from jax.experimental import pallas as pl
from jax.experimental.pallas import tpu as pltpu
from jax.sharding import PartitionSpec as P

MESH = pl.DeviceIdType.MESH
F32, BF16 = jnp.float32, jnp.bfloat16
PEERS = [(dy, dz) for dy in (2, 1, 3, 0) for dz in (1, 0) if (dy, dz) != (0, 0)]


class Spot:
    def __init__(self):
        dp, ep = lax.axis_index("dp"), lax.axis_index("ep")
        self.y, self.zl, self.c = dp // 4, (dp // 2) % 2, dp % 2
        self.zh, self.x = ep // 4, ep % 4
        self.b = self.block(0, 0)

    def to(self, y=0, zl=0, c=0, zh=0, x=0):
        dp = (self.y + y) % 4 * 4 + (self.zl + zl) % 2 * 2 + (self.c + c) % 2
        return (dp, (self.zh + zh) % 2 * 4 + (self.x + x) % 4)

    def block(self, y, zl):
        return (self.zl + zl) % 2 * 4 + (self.y + y) % 4

    def columns(self, y, zl, width=768, offset=0):
        start = ((self.y + y) % 4 * 2 + (self.zl + zl) % 2) * 768 + offset
        return pl.ds(pl.multiple_of(start, 128), width)

    def expert(self, x, zh):
        return (self.zh + zh) % 2 * 4 + (self.x + x) % 4


class Links:
    def __init__(self, send_sem, recv_sem):
        self.send_sem, self.recv_sem, self.count, self.sent = send_sem, recv_sem, 0, []

    def send(self, src, dst, device):
        n = self.count
        self.count += 1
        copy = pltpu.make_async_remote_copy(
            src_ref=src,
            dst_ref=dst,
            send_sem=self.send_sem.at[n],
            recv_sem=self.recv_sem.at[n],
            device_id=device,
            device_id_type=MESH,
        )
        copy.start()
        self.sent.append(copy)
        return copy

    def finish(self):
        assert self.count == self.send_sem.shape[0]
        for copy in self.sent:
            copy.wait_send()


def greet(devices):
    barrier = pltpu.get_barrier_semaphore()
    for device in devices:
        pl.semaphore_signal(barrier, inc=1, device_id=device, device_id_type=MESH)
    pl.semaphore_wait(barrier, len(devices))


def add_rows(dst, sources, rows, step=32):
    @pl.loop(0, rows // step)
    def _(i):
        at = pl.ds(pl.multiple_of(i * step, step), step)
        total = sources[0][at, :].astype(F32)
        for source in sources[1:]:
            total = total + source[at, :].astype(F32)
        dst[at, :] = total.astype(dst.dtype)


SPREAD_COPIES = 19 + 24 + 7


def spread_kernel(
    tok, og, ids_rows, gate_in, up_in, down_in, part, xt, ogt, idc, w_out,
    w_in, ids, x, g, ids_in, w, z_tok, z_og, l_tok, r_og, send_sem, recv_sem, own_sem, w_sem,
):
    me = Spot()
    right, left, up, down = me.to(x=1), me.to(x=3), me.to(y=1), me.to(y=3)
    core, far, pair = me.to(c=1), me.to(zh=1), me.to(zl=1)
    w_in[:, :256] = gate_in[...]
    w_in[:, 256:512] = up_in[...]
    w_in[:, 512:] = jnp.transpose(down_in[...])
    ids[...] = jnp.zeros((8, 128), jnp.int32)
    ids[:2, :] = ids_rows[...]
    greet([me.to(y=dy, zl=dz) for dy, dz in PEERS] + [right, left, core, far])
    links = Links(send_sem, recv_sem)
    own, far_e = me.expert(0, 0), me.expert(0, 1)

    from_far = links.send(w_in, w.at[own, me.c], far)
    from_left0 = links.send(w_in, w.at[own, me.c], right)
    from_right0 = links.send(w_in, w.at[own, me.c], left)
    from_core = {(0, 0): [links.send(w_in, w.at[own, me.c], core)]}

    def cut(array, y, zl):
        return array.at[:, me.columns(y, zl)]

    plane = [
        links.send(cut(tok, 2, 0), l_tok.at[0], up),
        links.send(cut(og, 2, 0), r_og.at[0], down),
    ]
    z_in = {}
    z_in[2, 0] = links.send(cut(tok, 2, 1), z_tok.at[2], pair)
    z_in[2, 1] = links.send(cut(og, 2, 1), z_og.at[2], pair)
    near = []
    for y, device in ((1, up), (3, down)):
        near.append(links.send(cut(tok, y, 0), x.at[me.b], device))
        near.append(links.send(cut(og, y, 0), g.at[me.b], device))
    for y in (1, 3):
        z_in[y, 0] = links.send(cut(tok, y, 1), z_tok.at[y], pair)
        z_in[y, 1] = links.send(cut(og, y, 1), z_og.at[y], pair)
    z_in[0, 0] = links.send(cut(tok, 0, 1), x.at[me.b], pair)
    z_in[0, 1] = links.send(cut(og, 0, 1), g.at[me.b], pair)
    names = [links.send(ids, ids_in.at[me.b], me.to(y=dy, zl=dz)) for dy, dz in PEERS]
    local = [
        pltpu.make_async_copy(w_in, w.at[own, me.c], own_sem.at[0]),
        pltpu.make_async_copy(cut(tok, 0, 0), x.at[me.b], own_sem.at[1]),
        pltpu.make_async_copy(cut(og, 0, 0), g.at[me.b], own_sem.at[2]),
        pltpu.make_async_copy(ids, ids_in.at[me.b], own_sem.at[3]),
    ]
    for copy in local:
        copy.start()

    @pl.loop(0, 64)
    def _(i):
        part[i // 8, pl.ds(pl.multiple_of(i % 8 * 32, 32), 32), :] = jnp.zeros((32, 768), BF16)

    def pass_on(expert, device, rows=pl.ds(0, 384)):
        piece = w.at[expert, me.c, rows, :]
        return links.send(piece, piece, device)

    low, high = pl.ds(0, 192), pl.ds(192, 192)
    across, ends = [], []
    z_in[2, 0].wait_recv()
    across.append(links.send(z_tok.at[2], l_tok.at[1], up))
    plane[0].wait_recv()
    ends.append(links.send(l_tok.at[0], x.at[me.block(3, 0)], up))
    z_in[2, 1].wait_recv()
    across.append(links.send(z_og.at[2], r_og.at[1], down))
    plane[1].wait_recv()
    ends.append(links.send(r_og.at[0], g.at[me.block(1, 0)], down))
    halves = {0: [], 1: []}

    def sideways(dz, from_left, from_right):
        from_left.wait_recv()
        halves[dz].append(pass_on(me.expert(3, dz), right, low))
        from_core[3, dz] = [pass_on(me.expert(3, dz), core)]
        from_right.wait_recv()
        halves[dz].append(pass_on(me.expert(1, dz), left, high))
        from_core[1, dz] = [pass_on(me.expert(1, dz), core)]

    sideways(0, from_left0, from_right0)
    late = []

    def partner(y, device):
        z_in[y, 0].wait_recv()
        late.append(links.send(z_tok.at[y], x.at[me.block(0, 1)], device))
        z_in[y, 1].wait_recv()
        late.append(links.send(z_og.at[y], g.at[me.block(0, 1)], device))

    partner(1, up)
    from_far.wait_recv()
    from_left1 = pass_on(far_e, right)
    from_right1 = pass_on(far_e, left)
    from_core[0, 1] = [pass_on(far_e, core)]
    partner(3, down)
    across[0].wait_recv()
    late.append(links.send(l_tok.at[1], x.at[me.block(3, 1)], up))
    across[1].wait_recv()
    late.append(links.send(r_og.at[1], g.at[me.block(1, 1)], down))

    def second(dz):
        from_core[2, dz] = []
        for n, half in enumerate(halves[dz]):
            half.wait_recv()
            from_core[2, dz].append(pass_on(me.expert(2, dz), core, (low, high)[n]))

    def turn(dz):
        for y in range(4):
            b = me.block(y, dz)
            at = pl.ds(pl.multiple_of(b * 128, 128), 128)
            xt[:, at] = jnp.transpose(x[b])
            ogt[:, at] = jnp.transpose(g[b])
            idc[at, :] = jnp.transpose(ids_in[b])

    def keep(step, dz):
        for copy in from_core[step, dz]:
            copy.wait_recv()
        e = me.expert(step, dz)
        pltpu.make_async_copy(w.at[e], w_out.at[e], w_sem.at[e]).start()

    def product(e, dz):
        plane_at = pl.multiple_of((me.zl + dz) % 2 * 4, 4)
        for n, source in ((0, x), (1, x), (2, g)):
            cols = slice(n * 256, n * 256 + 256)
            rows = source[pl.ds(plane_at, 4)].reshape(512, 768)
            out = jnp.dot(rows, w[e, :, :, cols].reshape(768, 256), preferred_element_type=F32)
            for y in range(4):
                names_at = pl.ds(pl.multiple_of((plane_at + y) * 128, 128), 128)
                for k in range(2):
                    here = part.at[plane_at + y, k * 128 : k * 128 + 128, cols]
                    chosen = idc[names_at, k : k + 1] == e
                    old = here[...].astype(F32)
                    here[...] = jnp.where(chosen, out[y * 128 : y * 128 + 128], old).astype(BF16)

    def first_six(i):
        g2 = i // 2
        step = (g2 + 1) // 2 * (1 + 2 * (i % 2))
        return me.expert(step, (1 - (g2 + 1) // 2) * (i % 2) + g2 // 2)

    for copy in near + ends + names:
        copy.wait_recv()
    for copy in local:
        copy.wait()
    turn(0)
    for step, dz in ((0, 0), (0, 1), (1, 0), (3, 0)):
        keep(step, dz)

    @pl.loop(0, 4)
    def _(i):
        product(first_six(i), 0)

    second(0)
    sideways(1, from_left1, from_right1)
    keep(1, 1)
    keep(3, 1)

    @pl.loop(4, 6)
    def _(i):
        product(first_six(i), 0)

    second(1)
    for copy in [z_in[0, 0], z_in[0, 1]] + late:
        copy.wait_recv()
    turn(1)

    @pl.loop(0, 6)
    def _(i):
        product(first_six(i), 1)

    keep(2, 0)
    keep(2, 1)

    @pl.loop(0, 4)
    def _(i):
        product(me.expert(2, i % 2), i // 2)

    links.finish()
    for e in range(8):
        pltpu.make_async_copy(w.at[e], w_out.at[e], w_sem.at[e]).wait()


def spread(tokens, out_grad, ids, w_gate, w_up, w_down):
    vmem, anywhere = pl.BlockSpec(memory_space=pltpu.VMEM), pl.BlockSpec(memory_space=pl.ANY)
    blocks = lambda n: pltpu.VMEM((n, 128, 768), BF16)
    return pl.pallas_call(
        spread_kernel,
        out_shape=(
            jax.ShapeDtypeStruct((8, 256, 768), BF16),
            jax.ShapeDtypeStruct((768, 1024), BF16),
            jax.ShapeDtypeStruct((768, 1024), BF16),
            jax.ShapeDtypeStruct((1024, 8), jnp.int32),
            jax.ShapeDtypeStruct((8, 2, 384, 768), BF16),
        ),
        in_specs=[vmem] * 6,
        out_specs=(vmem,) * 4 + (anywhere,),
        scratch_shapes=[
            pltpu.VMEM((384, 768), BF16),
            pltpu.VMEM((8, 128), jnp.int32),
            blocks(8),
            blocks(8),
            pltpu.VMEM((8, 8, 128), jnp.int32),
            pltpu.VMEM((8, 2, 384, 768), BF16),
            blocks(4),
            blocks(4),
            blocks(2),
            blocks(2),
            pltpu.SemaphoreType.DMA((SPREAD_COPIES,)),
            pltpu.SemaphoreType.DMA((SPREAD_COPIES,)),
            pltpu.SemaphoreType.DMA((4,)),
            pltpu.SemaphoreType.DMA((8,)),
        ],
        compiler_params=pltpu.CompilerParams(collective_id=0, has_side_effects=True, vmem_limit_bytes=60 << 20),
        name="spread",
    )(tokens, out_grad, ids, w_gate, w_up, w_down)


def activation(pre, weight):
    gate, up, grad_hidden = pre[:, :256], pre[:, 256:512], pre[:, 512:] * weight
    sig = jax.nn.sigmoid(gate)
    silu = gate * sig
    hidden = silu * up * weight
    grad_gate = grad_hidden * up * sig * (1.0 + gate * (1.0 - sig))
    grad_up = grad_hidden * silu
    return grad_gate.astype(BF16), grad_up.astype(BF16), hidden.astype(BF16)


MIDDLE_COPIES = 13 + 10 + 9 + 8


def middle_kernel(
    part, weight_rows, h_out, weight8, weight, ra, rb, sa, sb, fl, fr, zs, zr, zin, s2, s1, s3, ra2, rb2, sa2, sb2, fl2, fr2, own,
    send_sem, recv_sem, own_sem,
):
    me = Spot()
    right, left, pair = me.to(y=1), me.to(y=3), me.to(zl=1)
    weight8[...] = jnp.zeros((8, 128), F32)
    weight8[:2, :] = weight_rows[...]
    weight[...] = jnp.transpose(weight8[...])
    greet([right, left, pair])
    links = Links(send_sem, recv_sem)
    low, high = pl.ds(0, 64), pl.ds(64, 64)
    k0, k1, k1_low, k1_high = pl.ds(0, 128), pl.ds(128, 128), pl.ds(128, 64), pl.ds(192, 64)

    first_a, first_b, other_b, other_a, last_a, last_b, z_in = {}, {}, {}, {}, {}, {}, {}
    z_in[2] = links.send(part.at[me.block(2, 1), k1, :], zin.at[2], pair)
    for dz in (1, 0):
        first_a[dz] = links.send(part.at[me.block(2, dz), low, :], ra.at[dz], right)
        first_b[dz] = links.send(part.at[me.block(2, dz), high, :], rb.at[dz], left)
    for y in (1, 3, 0):
        z_in[y] = links.send(part.at[me.block(y, 1), k1, :], zin.at[y], pair)
    for dz in (1, 0):
        other_b[dz] = links.send(part.at[me.block(1, dz), high, :], fl.at[dz, high, :], right)
        other_a[dz] = links.send(part.at[me.block(3, dz), low, :], fr.at[dz, low, :], left)

    def relay(dz):
        first_a[dz].wait_recv()
        add_rows(sa.at[dz], [part.at[me.block(1, dz), low, :], ra.at[dz]], 64)
        last_a[dz] = links.send(sa.at[dz], fl.at[dz, low, :], right)
        first_b[dz].wait_recv()
        add_rows(sb.at[dz], [part.at[me.block(3, dz), high, :], rb.at[dz]], 64)
        last_b[dz] = links.send(sb.at[dz], fr.at[dz, high, :], left)

    relay(1)
    z_in[2].wait_recv()
    add_rows(s2, [part.at[me.block(2, 0), k1, :], zin.at[2]], 128)
    far_a = links.send(s2.at[low, :], ra2, right)
    far_b = links.send(s2.at[high, :], rb2, left)
    relay(0)
    z_in[1].wait_recv()
    add_rows(s1, [part.at[me.block(1, 0), k1_high, :], zin.at[1, high, :]], 64)
    side_b = links.send(s1, fl2.at[high, :], right)
    for group in (other_b, other_a, last_a, last_b):
        group[1].wait_recv()
    add_rows(zs, [part.at[me.block(0, 1), k0, :], fl.at[1], fr.at[1]], 128)
    cross = links.send(zs, zr, pair)
    z_in[3].wait_recv()
    add_rows(s3, [part.at[me.block(3, 0), k1_low, :], zin.at[3, low, :]], 64)
    side_a = links.send(s3, fr2.at[low, :], left)
    far_a.wait_recv()
    add_rows(sa2, [part.at[me.block(1, 0), k1_low, :], zin.at[1, low, :], ra2], 64)
    end_a = links.send(sa2, fl2.at[low, :], right)
    far_b.wait_recv()
    add_rows(sb2, [part.at[me.block(3, 0), k1_high, :], zin.at[3, high, :], rb2], 64)
    end_b = links.send(sb2, fr2.at[high, :], left)

    def active(k, sources):
        @pl.loop(0, 8)
        def _(i):
            row = pl.multiple_of(i * 16, 16)
            at = pl.ds(k * 128 + row, 16)
            pre = part[me.b, at, :].astype(F32)
            for source in sources:
                pre = pre + source[pl.ds(row, 16), :].astype(F32)
            own[at, :256], own[at, 256:512], own[at, 512:] = activation(pre, weight[pl.ds(row, 16), k : k + 1])

    for group in (other_b, other_a, last_a, last_b):
        group[0].wait_recv()
    cross.wait_recv()
    active(0, [fl.at[0], fr.at[0], zr])
    mine0 = pltpu.make_async_copy(own.at[k0, :], h_out.at[me.b, k0, :], own_sem.at[0])
    mine0.start()
    from_pair = links.send(own.at[k0, :], h_out.at[me.b, k0, :], pair)
    from_left = {0: links.send(own.at[k0, :], h_out.at[me.b, k0, :], right)}
    from_right = {0: links.send(own.at[k0, :], h_out.at[me.b, k0, :], left)}

    def pass_on(block, device, rows):
        piece = h_out.at[block, rows, :]
        return links.send(piece, piece, device)

    for copy in (z_in[0], side_a, side_b, end_a, end_b):
        copy.wait_recv()
    active(1, [zin.at[0], fl2, fr2])
    mine1 = pltpu.make_async_copy(own.at[k1, :], h_out.at[me.b, k1, :], own_sem.at[1])
    mine1.start()
    left1 = links.send(own.at[k1, :], h_out.at[me.b, k1, :], right)
    right1 = links.send(own.at[k1, :], h_out.at[me.b, k1, :], left)
    tail = [links.send(own.at[k1, :], h_out.at[me.b, k1, :], pair)]
    from_pair.wait_recv()
    from_left[1] = pass_on(me.block(0, 1), right, k0)
    from_right[1] = pass_on(me.block(0, 1), left, k0)
    from_left[0].wait_recv()
    tail.append(pass_on(me.block(3, 0), right, low))
    from_right[0].wait_recv()
    tail.append(pass_on(me.block(1, 0), left, high))
    left1.wait_recv()
    half_a = pass_on(me.block(3, 0), right, k1_low)
    tail.append(pass_on(me.block(3, 0), pair, k1))
    right1.wait_recv()
    half_b = pass_on(me.block(1, 0), left, k1_high)
    tail.append(pass_on(me.block(1, 0), pair, k1))
    from_left[1].wait_recv()
    tail.append(pass_on(me.block(3, 1), right, low))
    from_right[1].wait_recv()
    tail.append(pass_on(me.block(1, 1), left, high))
    half_a.wait_recv()
    half_b.wait_recv()
    tail.append(pass_on(me.block(2, 0), pair, k1))
    for copy in tail:
        copy.wait_recv()
    mine0.wait()
    mine1.wait()
    links.finish()


def middle(part, weight):
    vmem, anywhere = pl.BlockSpec(memory_space=pltpu.VMEM), pl.BlockSpec(memory_space=pl.ANY)
    rows = lambda *shape: pltpu.VMEM(shape + (768,), BF16)
    return pl.pallas_call(
        middle_kernel,
        out_shape=jax.ShapeDtypeStruct((8, 256, 768), BF16),
        in_specs=[vmem] * 2,
        out_specs=anywhere,
        scratch_shapes=[pltpu.VMEM((8, 128), F32), pltpu.VMEM((128, 8), F32)]
        + [rows(2, 64)] * 4
        + [rows(2, 128)] * 2
        + [rows(128)] * 2
        + [rows(4, 128), rows(128)]
        + [rows(64)] * 6
        + [rows(128)] * 2
        + [
            rows(256),
            pltpu.SemaphoreType.DMA((MIDDLE_COPIES,)),
            pltpu.SemaphoreType.DMA((MIDDLE_COPIES,)),
            pltpu.SemaphoreType.DMA((2,)),
        ],
        compiler_params=pltpu.CompilerParams(collective_id=1, has_side_effects=True),
        name="middle",
    )(part, weight)


FINISH_COPIES = 7 + 8 + 4 + 4 + 4 + 1
ORDER = ((2, 1), (1, 1), (3, 1), (2, 0), (1, 0), (3, 0), (0, 1), (0, 0))


def finish_kernel(
    xt, ogt, ids, h, w, d_out, gate_out, up_out, down_out,
    w_all, he, g, cr, dx, g_out, a2, ra, rb, sa, sb, oa, ob, fl, fr, zs, zr,
    send_sem, recv_sem, w_sem, own_sem,
):
    me = Spot()
    right, left, core, far = me.to(x=1), me.to(x=3), me.to(c=1), me.to(zh=1)
    loads = [pltpu.make_async_copy(w.at[e], w_all.at[e], w_sem.at[e]) for e in range(8)]
    for load in loads:
        load.start()
    greet([me.to(y=dy, zl=dz) for dy, dz in PEERS] + [right, left, core, far])
    links = Links(send_sem, recv_sem)
    low, high = pl.ds(0, 192), pl.ds(192, 192)
    mine, others = me.c, 1 - me.c
    swapped, first_a, first_b, other_b, other_a, last_a, last_b = {}, {}, {}, {}, {}, {}, {}

    def product(step, dz):
        e = me.expert(step, dz)

        @pl.loop(0, 8)
        def _(q):
            at = pl.ds(pl.multiple_of(q * 128, 128), 128)
            chosen = [(ids[at, k : k + 1] == e).astype(F32) for k in range(2)]
            m0, m1 = [jnp.broadcast_to(m, (128, 128)).astype(BF16) for m in chosen]
            for n in range(6):
                cols = slice(n * 128, n * 128 + 128)
                he[e, at, cols] = h[q, :128, cols] * m0 + h[q, 128:, cols] * m1

        for n, left_t in ((0, xt), (1, xt), (2, ogt)):
            cols = slice(n * 256, n * 256 + 256)
            out = jnp.dot(left_t[...], he[e, :, cols], preferred_element_type=F32).astype(BF16)
            g[e, 0, :, cols] = out[:384]
            g[e, 1, :, cols] = out[384:]
        swapped[step, dz] = links.send(g.at[e, others], cr.at[e], core)

    def start_far(dz):
        e = me.expert(2, dz)
        swapped[2, dz].wait_recv()
        add_rows(a2.at[dz], [g.at[e, mine], cr.at[e]], 384)
        first_a[dz] = links.send(a2.at[dz, low, :], ra.at[dz], right)
        first_b[dz] = links.send(a2.at[dz, high, :], rb.at[dz], left)

    def start_near(dz):
        e = me.expert(1, dz)
        swapped[1, dz].wait_recv()
        add_rows(ob.at[dz], [g.at[e, mine, high, :], cr.at[e, high, :]], 192)
        other_b[dz] = links.send(ob.at[dz], fl.at[dz, high, :], right)
        e = me.expert(3, dz)
        swapped[3, dz].wait_recv()
        add_rows(oa.at[dz], [g.at[e, mine, low, :], cr.at[e, low, :]], 192)
        other_a[dz] = links.send(oa.at[dz], fr.at[dz, low, :], left)

    def relay(dz):
        e = me.expert(1, dz)
        first_a[dz].wait_recv()
        add_rows(sa.at[dz], [g.at[e, mine, low, :], cr.at[e, low, :], ra.at[dz]], 192)
        last_a[dz] = links.send(sa.at[dz], fl.at[dz, low, :], right)
        e = me.expert(3, dz)
        first_b[dz].wait_recv()
        add_rows(sb.at[dz], [g.at[e, mine, high, :], cr.at[e, high, :], rb.at[dz]], 192)
        last_b[dz] = links.send(sb.at[dz], fr.at[dz, high, :], left)

    def token_part(n):
        cols = slice(n * 256, n * 256 + 256)
        total = None
        for e in range(8):
            part = lax.dot_general(
                he[e, :, :512], w_all[e, cols, :512], (((1,), (1,)), ((), ())), preferred_element_type=F32
            )
            total = part if total is None else total + part
        for q in range(8):
            dx[q, :, cols] = total[q * 128 : q * 128 + 128].astype(BF16)

    product(2, 1)
    product(1, 1)
    start_far(1)
    product(3, 1)
    product(2, 0)
    start_near(1)
    product(1, 0)
    start_far(0)
    product(3, 0)
    product(0, 1)
    start_near(0)
    relay(1)
    product(0, 0)
    for load in loads:
        load.wait()
    token_part(0)
    token_part(1)
    token_part(2)
    back = []
    cols = me.columns(0, 0)
    for dy, dz in PEERS:
        back.append(links.send(dx.at[me.block(dy, dz)], d_out.at[:, cols], me.to(y=dy, zl=dz)))
    keep = pltpu.make_async_copy(dx.at[me.b], d_out.at[:, cols], own_sem)
    keep.start()
    relay(0)
    for group in (other_b, other_a, last_a, last_b):
        group[1].wait_recv()
    e = me.expert(0, 1)
    swapped[0, 1].wait_recv()
    add_rows(zs, [g.at[e, mine], cr.at[e], fl.at[1], fr.at[1]], 384)
    cross = links.send(zs, zr, far)
    for group in (other_b, other_a, last_a, last_b):
        group[0].wait_recv()
    swapped[0, 0].wait_recv()
    cross.wait_recv()
    e = me.expert(0, 0)
    add_rows(g_out, [g.at[e, mine], cr.at[e], fl.at[0], fr.at[0], zr], 384)
    gate_out[...] = g_out[:, :256]
    up_out[...] = g_out[:, 256:512]
    down_out[...] = jnp.transpose(g_out[:, 512:])
    for copy in back:
        copy.wait_recv()
    keep.wait()
    links.finish()


def finish(xt, ogt, ids, h, w):
    vmem, anywhere = pl.BlockSpec(memory_space=pltpu.VMEM), pl.BlockSpec(memory_space=pl.ANY)
    half, full = pltpu.VMEM((2, 192, 768), BF16), pltpu.VMEM((2, 384, 768), BF16)
    one = pltpu.VMEM((384, 768), BF16)
    return pl.pallas_call(
        finish_kernel,
        out_shape=(
            jax.ShapeDtypeStruct((128, 6144), BF16),
            jax.ShapeDtypeStruct((384, 256), F32),
            jax.ShapeDtypeStruct((384, 256), F32),
            jax.ShapeDtypeStruct((256, 384), F32),
        ),
        in_specs=[vmem] * 4 + [anywhere],
        out_specs=(anywhere,) + (vmem,) * 3,
        scratch_shapes=[
            pltpu.VMEM((8, 768, 768), BF16),
            pltpu.VMEM((8, 1024, 768), BF16),
            pltpu.VMEM((8, 2, 384, 768), BF16),
            pltpu.VMEM((8, 384, 768), BF16),
            pltpu.VMEM((8, 128, 768), BF16),
            pltpu.VMEM((384, 768), F32),
        ]
        + [full] + [half] * 6 + [full] * 2 + [one] * 2
        + [
            pltpu.SemaphoreType.DMA((FINISH_COPIES,)),
            pltpu.SemaphoreType.DMA((FINISH_COPIES,)),
            pltpu.SemaphoreType.DMA((8,)),
            pltpu.SemaphoreType.DMA,
        ],
        compiler_params=pltpu.CompilerParams(collective_id=2, has_side_effects=True, vmem_limit_bytes=60 << 20),
        name="finish",
    )(xt, ogt, ids, h, w)


def shards(tokens, out_grad, expert_ids, route_weight, w_gate, w_up, w_down):
    part, xt, ogt, names, w = spread(tokens, out_grad, jnp.transpose(expert_ids), w_gate[0], w_up[0], w_down[0])
    h = middle(part, jnp.transpose(route_weight))
    d_tokens, gate, up, down = finish(xt, ogt, names, h, w.reshape(8, 768, 768))
    return d_tokens, gate[None], up[None], down[None]


def solution(mesh):
    in_specs = (
        P(("dp", "ep"), None),
        P(("dp", "ep"), None),
        P(("dp", "ep"), None),
        P(("dp", "ep"), None),
        P("ep", "dp", None),
        P("ep", "dp", None),
        P("ep", None, "dp"),
    )
    out_specs = (
        P(("dp", "ep"), None),
        P("ep", "dp", None),
        P("ep", "dp", None),
        P("ep", None, "dp"),
    )
    return jax.shard_map(shards, mesh=mesh, in_specs=in_specs, out_specs=out_specs, check_vma=False)
```

```python
import functools

import jax
import jax.numpy as jnp
from jax import lax
from jax.experimental import pallas as pl
from jax.experimental.pallas import tpu as pltpu
from jax.sharding import PartitionSpec as P

MESH = pl.DeviceIdType.MESH
F32, BF16 = jnp.float32, jnp.bfloat16
PEERS = [(dy, dz) for dy in (2, 1, 3, 0) for dz in (1, 0) if (dy, dz) != (0, 0)]


class Spot:
    def __init__(self):
        dp, ep = lax.axis_index("dp"), lax.axis_index("ep")
        self.y, self.zl, self.c = dp // 4, (dp // 2) % 2, dp % 2
        self.zh, self.x = ep // 4, ep % 4
        self.b = self.block(0, 0)

    def to(self, y=0, zl=0, c=0, zh=0, x=0):
        dp = (self.y + y) % 4 * 4 + (self.zl + zl) % 2 * 2 + (self.c + c) % 2
        return (dp, (self.zh + zh) % 2 * 4 + (self.x + x) % 4)

    def block(self, y, zl):
        return (self.zl + zl) % 2 * 4 + (self.y + y) % 4

    def columns(self, y, zl, width=768, offset=0):
        start = ((self.y + y) % 4 * 2 + (self.zl + zl) % 2) * 768 + offset
        return pl.ds(pl.multiple_of(start, 128), width)

    def expert(self, x, zh):
        return (self.zh + zh) % 2 * 4 + (self.x + x) % 4


class Links:
    def __init__(self, send_sem, recv_sem):
        self.send_sem, self.recv_sem, self.count, self.sent = send_sem, recv_sem, 0, []

    def send(self, src, dst, device):
        n = self.count
        self.count += 1
        copy = pltpu.make_async_remote_copy(
            src_ref=src,
            dst_ref=dst,
            send_sem=self.send_sem.at[n],
            recv_sem=self.recv_sem.at[n],
            device_id=device,
            device_id_type=MESH,
        )
        copy.start()
        self.sent.append(copy)
        return copy

    def finish(self):
        assert self.count == self.send_sem.shape[0]
        for copy in self.sent:
            copy.wait_send()


def greet(devices):
    barrier = pltpu.get_barrier_semaphore()
    for device in devices:
        pl.semaphore_signal(barrier, inc=1, device_id=device, device_id_type=MESH)
    pl.semaphore_wait(barrier, len(devices))


def add_rows(dst, sources, rows, step=32):
    @pl.loop(0, rows // step)
    def _(i):
        at = pl.ds(pl.multiple_of(i * step, step), step)
        total = sources[0][at, :].astype(F32)
        for source in sources[1:]:
            total = total + source[at, :].astype(F32)
        dst[at, :] = total.astype(dst.dtype)


def activation(pre, weight):
    gate, up, grad_hidden = pre[:, :256], pre[:, 256:512], pre[:, 512:] * weight
    sig = jax.nn.sigmoid(gate)
    silu = gate * sig
    hidden = silu * up * weight
    grad_gate = grad_hidden * up * sig * (1.0 + gate * (1.0 - sig))
    grad_up = grad_hidden * silu
    return grad_gate.astype(BF16), grad_up.astype(BF16), hidden.astype(BF16)


def open_sums(me, links, part, dz, sums):
    ra, rb, fl, fr = sums[2], sums[3], sums[6], sums[7]
    right, left = me.to(y=1), me.to(y=3)
    low, high = pl.ds(0, 64), pl.ds(64, 64)
    return (
        links.send(part.at[me.block(2, dz), low, :], ra.at[dz], right),
        links.send(part.at[me.block(2, dz), high, :], rb.at[dz], left),
        links.send(part.at[me.block(1, dz), high, :], fl.at[dz, high, :], right),
        links.send(part.at[me.block(3, dz), low, :], fr.at[dz, low, :], left),
    )


def close_sums(me, links, part, weight_rows, h_out, opened, sums):
    (
        weight8, weight, ra, rb, sa, sb, fl, fr, zs, zr, zin, s2, s1, s3, ra2, rb2, sa2, sb2, fl2, fr2, own, h_sem,
    ) = sums
    right, left, pair = me.to(y=1), me.to(y=3), me.to(zl=1)
    low, high = pl.ds(0, 64), pl.ds(64, 64)
    k0, k1, k1_low, k1_high = pl.ds(0, 128), pl.ds(128, 128), pl.ds(128, 64), pl.ds(192, 64)
    z_in = {2: links.send(part.at[me.block(2, 1), k1, :], zin.at[2], pair)}
    opened[1] = open_sums(me, links, part, 1, sums)
    first_a, first_b, other_b, other_a = [{dz: opened[dz][n] for dz in (0, 1)} for n in range(4)]
    last_a, last_b = {}, {}
    for y in (1, 3, 0):
        z_in[y] = links.send(part.at[me.block(y, 1), k1, :], zin.at[y], pair)
    weight8[...] = jnp.zeros((8, 128), F32)
    weight8[:2, :] = weight_rows[...]
    weight[...] = jnp.transpose(weight8[...])

    def relay(dz):
        first_a[dz].wait_recv()
        add_rows(sa.at[dz], [part.at[me.block(1, dz), low, :], ra.at[dz]], 64)
        last_a[dz] = links.send(sa.at[dz], fl.at[dz, low, :], right)
        first_b[dz].wait_recv()
        add_rows(sb.at[dz], [part.at[me.block(3, dz), high, :], rb.at[dz]], 64)
        last_b[dz] = links.send(sb.at[dz], fr.at[dz, high, :], left)

    relay(0)
    relay(1)
    z_in[2].wait_recv()
    add_rows(s2, [part.at[me.block(2, 0), k1, :], zin.at[2]], 128)
    far_a = links.send(s2.at[low, :], ra2, right)
    far_b = links.send(s2.at[high, :], rb2, left)
    z_in[1].wait_recv()
    add_rows(s1, [part.at[me.block(1, 0), k1_high, :], zin.at[1, high, :]], 64)
    side_b = links.send(s1, fl2.at[high, :], right)
    for group in (other_b, other_a, last_a, last_b):
        group[1].wait_recv()
    add_rows(zs, [part.at[me.block(0, 1), k0, :], fl.at[1], fr.at[1]], 128)
    cross = links.send(zs, zr, pair)
    z_in[3].wait_recv()
    add_rows(s3, [part.at[me.block(3, 0), k1_low, :], zin.at[3, low, :]], 64)
    side_a = links.send(s3, fr2.at[low, :], left)
    far_a.wait_recv()
    add_rows(sa2, [part.at[me.block(1, 0), k1_low, :], zin.at[1, low, :], ra2], 64)
    end_a = links.send(sa2, fl2.at[low, :], right)
    far_b.wait_recv()
    add_rows(sb2, [part.at[me.block(3, 0), k1_high, :], zin.at[3, high, :], rb2], 64)
    end_b = links.send(sb2, fr2.at[high, :], left)

    def active(k, sources):
        @pl.loop(0, 8)
        def _(i):
            row = pl.multiple_of(i * 16, 16)
            at = pl.ds(k * 128 + row, 16)
            pre = part[me.b, at, :].astype(F32)
            for source in sources:
                pre = pre + source[pl.ds(row, 16), :].astype(F32)
            own[at, :256], own[at, 256:512], own[at, 512:] = activation(pre, weight[pl.ds(row, 16), k : k + 1])

    for group in (other_b, other_a, last_a, last_b):
        group[0].wait_recv()
    cross.wait_recv()
    active(0, [fl.at[0], fr.at[0], zr])
    mine0 = pltpu.make_async_copy(own.at[k0, :], h_out.at[me.b, k0, :], h_sem.at[0])
    mine0.start()
    from_pair = links.send(own.at[k0, :], h_out.at[me.b, k0, :], pair)
    from_left = {0: links.send(own.at[k0, :], h_out.at[me.b, k0, :], right)}
    from_right = {0: links.send(own.at[k0, :], h_out.at[me.b, k0, :], left)}

    def pass_on(block, device, rows):
        piece = h_out.at[block, rows, :]
        return links.send(piece, piece, device)

    for copy in (z_in[0], side_a, side_b, end_a, end_b):
        copy.wait_recv()
    active(1, [zin.at[0], fl2, fr2])
    mine1 = pltpu.make_async_copy(own.at[k1, :], h_out.at[me.b, k1, :], h_sem.at[1])
    mine1.start()
    left1 = links.send(own.at[k1, :], h_out.at[me.b, k1, :], right)
    right1 = links.send(own.at[k1, :], h_out.at[me.b, k1, :], left)
    tail = [links.send(own.at[k1, :], h_out.at[me.b, k1, :], pair)]
    from_pair.wait_recv()
    from_left[1] = pass_on(me.block(0, 1), right, k0)
    from_right[1] = pass_on(me.block(0, 1), left, k0)
    from_left[0].wait_recv()
    tail.append(pass_on(me.block(3, 0), right, low))
    from_right[0].wait_recv()
    tail.append(pass_on(me.block(1, 0), left, high))
    left1.wait_recv()
    half_a = pass_on(me.block(3, 0), right, k1_low)
    tail.append(pass_on(me.block(3, 0), pair, k1))
    right1.wait_recv()
    half_b = pass_on(me.block(1, 0), left, k1_high)
    tail.append(pass_on(me.block(1, 0), pair, k1))
    from_left[1].wait_recv()
    tail.append(pass_on(me.block(3, 1), right, low))
    from_right[1].wait_recv()
    tail.append(pass_on(me.block(1, 1), left, high))
    half_a.wait_recv()
    half_b.wait_recv()
    tail.append(pass_on(me.block(2, 0), pair, k1))
    for copy in tail:
        copy.wait_recv()
    mine0.wait()
    mine1.wait()


FORWARD_COPIES = 19 + 24 + 7 + 40


def forward_kernel(
    tok, og, ids_rows, weight_rows, gate_in, up_in, down_in, h_out, xt, ogt, idc, w_out,
    part, w_in, ids, x, g, ids_in, w, z_tok, z_og, l_tok, r_og, send_sem, recv_sem, own_sem, w_sem, *sums
):
    me = Spot()
    right, left, up, down = me.to(x=1), me.to(x=3), me.to(y=1), me.to(y=3)
    core, far, pair = me.to(c=1), me.to(zh=1), me.to(zl=1)
    w_in[:, :256] = gate_in[...]
    w_in[:, 256:512] = up_in[...]
    w_in[:, 512:] = jnp.transpose(down_in[...])
    ids[...] = jnp.zeros((8, 128), jnp.int32)
    ids[:2, :] = ids_rows[...]
    greet([me.to(y=dy, zl=dz) for dy, dz in PEERS] + [right, left, core, far])
    links = Links(send_sem, recv_sem)
    own, far_e = me.expert(0, 0), me.expert(0, 1)

    from_far = links.send(w_in, w.at[own, me.c], far)
    from_left0 = links.send(w_in, w.at[own, me.c], right)
    from_right0 = links.send(w_in, w.at[own, me.c], left)
    from_core = {(0, 0): [links.send(w_in, w.at[own, me.c], core)]}

    def cut(array, y, zl):
        return array.at[:, me.columns(y, zl)]

    plane = [
        links.send(cut(tok, 2, 0), l_tok.at[0], up),
        links.send(cut(og, 2, 0), r_og.at[0], down),
    ]
    z_in = {}
    z_in[2, 0] = links.send(cut(tok, 2, 1), z_tok.at[2], pair)
    z_in[2, 1] = links.send(cut(og, 2, 1), z_og.at[2], pair)
    near = []
    for y, device in ((1, up), (3, down)):
        near.append(links.send(cut(tok, y, 0), x.at[me.b], device))
        near.append(links.send(cut(og, y, 0), g.at[me.b], device))
    for y in (1, 3):
        z_in[y, 0] = links.send(cut(tok, y, 1), z_tok.at[y], pair)
        z_in[y, 1] = links.send(cut(og, y, 1), z_og.at[y], pair)
    z_in[0, 0] = links.send(cut(tok, 0, 1), x.at[me.b], pair)
    z_in[0, 1] = links.send(cut(og, 0, 1), g.at[me.b], pair)
    names = [links.send(ids, ids_in.at[me.b], me.to(y=dy, zl=dz)) for dy, dz in PEERS]
    local = [
        pltpu.make_async_copy(w_in, w.at[own, me.c], own_sem.at[0]),
        pltpu.make_async_copy(cut(tok, 0, 0), x.at[me.b], own_sem.at[1]),
        pltpu.make_async_copy(cut(og, 0, 0), g.at[me.b], own_sem.at[2]),
        pltpu.make_async_copy(ids, ids_in.at[me.b], own_sem.at[3]),
    ]
    for copy in local:
        copy.start()

    @pl.loop(0, 64)
    def _(i):
        part[i // 8, pl.ds(pl.multiple_of(i % 8 * 32, 32), 32), :] = jnp.zeros((32, 768), BF16)

    def pass_on(expert, device, rows=pl.ds(0, 384)):
        piece = w.at[expert, me.c, rows, :]
        return links.send(piece, piece, device)

    low, high = pl.ds(0, 192), pl.ds(192, 192)
    across, ends = [], []
    z_in[2, 0].wait_recv()
    across.append(links.send(z_tok.at[2], l_tok.at[1], up))
    plane[0].wait_recv()
    ends.append(links.send(l_tok.at[0], x.at[me.block(3, 0)], up))
    z_in[2, 1].wait_recv()
    across.append(links.send(z_og.at[2], r_og.at[1], down))
    plane[1].wait_recv()
    ends.append(links.send(r_og.at[0], g.at[me.block(1, 0)], down))
    halves = {0: [], 1: []}

    def sideways(dz, from_left, from_right):
        from_left.wait_recv()
        halves[dz].append(pass_on(me.expert(3, dz), right, low))
        from_core[3, dz] = [pass_on(me.expert(3, dz), core)]
        from_right.wait_recv()
        halves[dz].append(pass_on(me.expert(1, dz), left, high))
        from_core[1, dz] = [pass_on(me.expert(1, dz), core)]

    sideways(0, from_left0, from_right0)
    late = []

    def partner(y, device):
        z_in[y, 0].wait_recv()
        late.append(links.send(z_tok.at[y], x.at[me.block(0, 1)], device))
        z_in[y, 1].wait_recv()
        late.append(links.send(z_og.at[y], g.at[me.block(0, 1)], device))

    partner(1, up)
    from_far.wait_recv()
    from_left1 = pass_on(far_e, right)
    from_right1 = pass_on(far_e, left)
    from_core[0, 1] = [pass_on(far_e, core)]
    partner(3, down)
    across[0].wait_recv()
    late.append(links.send(l_tok.at[1], x.at[me.block(3, 1)], up))
    across[1].wait_recv()
    late.append(links.send(r_og.at[1], g.at[me.block(1, 1)], down))

    def second(dz):
        from_core[2, dz] = []
        for n, half in enumerate(halves[dz]):
            half.wait_recv()
            from_core[2, dz].append(pass_on(me.expert(2, dz), core, (low, high)[n]))

    def turn(dz):
        for y in range(4):
            b = me.block(y, dz)
            at = pl.ds(pl.multiple_of(b * 128, 128), 128)
            xt[:, at] = jnp.transpose(x[b])
            ogt[:, at] = jnp.transpose(g[b])
            idc[at, :] = jnp.transpose(ids_in[b])

    def keep(step, dz):
        for copy in from_core[step, dz]:
            copy.wait_recv()
        e = me.expert(step, dz)
        pltpu.make_async_copy(w.at[e], w_out.at[e], w_sem.at[e]).start()

    def product(e, dz):
        plane_at = pl.multiple_of((me.zl + dz) % 2 * 4, 4)
        for n, source in ((0, x), (1, x), (2, g)):
            cols = slice(n * 256, n * 256 + 256)
            rows = source[pl.ds(plane_at, 4)].reshape(512, 768)
            out = jnp.dot(rows, w[e, :, :, cols].reshape(768, 256), preferred_element_type=F32)
            for y in range(4):
                names_at = pl.ds(pl.multiple_of((plane_at + y) * 128, 128), 128)
                for k in range(2):
                    here = part.at[plane_at + y, k * 128 : k * 128 + 128, cols]
                    chosen = idc[names_at, k : k + 1] == e
                    old = here[...].astype(F32)
                    here[...] = jnp.where(chosen, out[y * 128 : y * 128 + 128], old).astype(BF16)

    def first_six(i):
        g2 = i // 2
        step = (g2 + 1) // 2 * (1 + 2 * (i % 2))
        return me.expert(step, (1 - (g2 + 1) // 2) * (i % 2) + g2 // 2)

    for copy in near + ends + names:
        copy.wait_recv()
    for copy in local:
        copy.wait()
    turn(0)
    for step, dz in ((0, 0), (0, 1), (1, 0), (3, 0)):
        keep(step, dz)

    @pl.loop(0, 4)
    def _(i):
        product(first_six(i), 0)

    second(0)
    sideways(1, from_left1, from_right1)
    keep(1, 1)
    keep(3, 1)

    @pl.loop(4, 6)
    def _(i):
        product(first_six(i), 0)

    second(1)
    keep(2, 0)
    keep(2, 1)

    @pl.loop(0, 2)
    def _(i):
        product(me.expert(2, i), 0)

    opened = {0: open_sums(me, links, part, 0, sums)}
    for copy in [z_in[0, 0], z_in[0, 1]] + late:
        copy.wait_recv()
    turn(1)

    @pl.loop(0, 8)
    def _(i):
        product(i, 1)

    close_sums(me, links, part, weight_rows, h_out, opened, sums)
    links.finish()
    for e in range(8):
        pltpu.make_async_copy(w.at[e], w_out.at[e], w_sem.at[e]).wait()


def forward(tokens, out_grad, ids, weight, w_gate, w_up, w_down):
    vmem, anywhere = pl.BlockSpec(memory_space=pltpu.VMEM), pl.BlockSpec(memory_space=pl.ANY)
    blocks = lambda n: pltpu.VMEM((n, 128, 768), BF16)
    rows = lambda *shape: pltpu.VMEM(shape + (768,), BF16)
    return pl.pallas_call(
        forward_kernel,
        out_shape=(
            jax.ShapeDtypeStruct((8, 256, 768), BF16),
            jax.ShapeDtypeStruct((768, 1024), BF16),
            jax.ShapeDtypeStruct((768, 1024), BF16),
            jax.ShapeDtypeStruct((1024, 8), jnp.int32),
            jax.ShapeDtypeStruct((8, 2, 384, 768), BF16),
        ),
        in_specs=[vmem] * 7,
        out_specs=(anywhere,) + (vmem,) * 3 + (anywhere,),
        scratch_shapes=[
            pltpu.VMEM((8, 256, 768), BF16),
            pltpu.VMEM((384, 768), BF16),
            pltpu.VMEM((8, 128), jnp.int32),
            blocks(8),
            blocks(8),
            pltpu.VMEM((8, 8, 128), jnp.int32),
            pltpu.VMEM((8, 2, 384, 768), BF16),
            blocks(4),
            blocks(4),
            blocks(2),
            blocks(2),
            pltpu.SemaphoreType.DMA((FORWARD_COPIES,)),
            pltpu.SemaphoreType.DMA((FORWARD_COPIES,)),
            pltpu.SemaphoreType.DMA((4,)),
            pltpu.SemaphoreType.DMA((8,)),
            pltpu.VMEM((8, 128), F32),
            pltpu.VMEM((128, 8), F32),
        ]
        + [rows(2, 64)] * 4
        + [rows(2, 128)] * 2
        + [rows(128)] * 2
        + [rows(4, 128), rows(128)]
        + [rows(64)] * 6
        + [rows(128)] * 2
        + [rows(256), pltpu.SemaphoreType.DMA((2,))],
        compiler_params=pltpu.CompilerParams(collective_id=0, has_side_effects=True, vmem_limit_bytes=60 << 20),
        name="forward",
    )(tokens, out_grad, ids, weight, w_gate, w_up, w_down)


FINISH_COPIES = 8 + 4 + 4 + 4 + 1 + 16


def finish_kernel(
    xt, ogt, ids, h, w, d_out, gate_out, up_out, down_out,
    w_all, he, g, cr, dx, g_out, zd, dl, dr, a2, ra, rb, sa, sb, oa, ob, fl, fr, zs, zr,
    send_sem, recv_sem, w_sem, own_sem,
):
    me = Spot()
    right, left, core, far = me.to(x=1), me.to(x=3), me.to(c=1), me.to(zh=1)
    up, down, pair = me.to(y=1), me.to(y=3), me.to(zl=1)
    loads = [pltpu.make_async_copy(w.at[e], w_all.at[e], w_sem.at[e]) for e in range(8)]
    for load in loads:
        load.start()
    greet([up, down, pair, right, left, core, far])
    links = Links(send_sem, recv_sem)
    low, high = pl.ds(0, 192), pl.ds(192, 192)
    mine, others = me.c, 1 - me.c
    swapped, first_a, first_b, other_b, other_a, last_a, last_b = {}, {}, {}, {}, {}, {}, {}

    def fill(step, dz):
        e = me.expert(step, dz)

        @pl.loop(0, 8)
        def _(q):
            at = pl.ds(pl.multiple_of(q * 128, 128), 128)
            chosen = [(ids[at, k : k + 1] == e).astype(F32) for k in range(2)]
            m0, m1 = [jnp.broadcast_to(m, (128, 128)).astype(BF16) for m in chosen]
            for n in range(6):
                cols = slice(n * 128, n * 128 + 128)
                he[e, at, cols] = h[q, :128, cols] * m0 + h[q, 128:, cols] * m1

    def product(step, dz):
        e = me.expert(step, dz)
        for n, left_t in ((0, xt), (1, xt), (2, ogt)):
            cols = slice(n * 256, n * 256 + 256)
            out = jnp.dot(left_t[...], he[e, :, cols], preferred_element_type=F32).astype(BF16)
            g[e, 0, :, cols] = out[:384]
            g[e, 1, :, cols] = out[384:]
        swapped[step, dz] = links.send(g.at[e, others], cr.at[e], core)

    def start_far(dz):
        e = me.expert(2, dz)
        swapped[2, dz].wait_recv()
        add_rows(a2.at[dz], [g.at[e, mine], cr.at[e]], 384)
        first_a[dz] = links.send(a2.at[dz, low, :], ra.at[dz], right)
        first_b[dz] = links.send(a2.at[dz, high, :], rb.at[dz], left)

    def start_near(dz):
        e = me.expert(1, dz)
        swapped[1, dz].wait_recv()
        add_rows(ob.at[dz], [g.at[e, mine, high, :], cr.at[e, high, :]], 192)
        other_b[dz] = links.send(ob.at[dz], fl.at[dz, high, :], right)
        e = me.expert(3, dz)
        swapped[3, dz].wait_recv()
        add_rows(oa.at[dz], [g.at[e, mine, low, :], cr.at[e, low, :]], 192)
        other_a[dz] = links.send(oa.at[dz], fr.at[dz, low, :], left)

    def relay(dz):
        e = me.expert(1, dz)
        first_a[dz].wait_recv()
        add_rows(sa.at[dz], [g.at[e, mine, low, :], cr.at[e, low, :], ra.at[dz]], 192)
        last_a[dz] = links.send(sa.at[dz], fl.at[dz, low, :], right)
        e = me.expert(3, dz)
        first_b[dz].wait_recv()
        add_rows(sb.at[dz], [g.at[e, mine, high, :], cr.at[e, high, :], rb.at[dz]], 192)
        last_b[dz] = links.send(sb.at[dz], fr.at[dz, high, :], left)

    def token_part(n):
        cols = slice(n * 256, n * 256 + 256)
        total = None
        for e in range(8):
            part = lax.dot_general(
                he[e, :, :512], w_all[e, cols, :512], (((1,), (1,)), ((), ())), preferred_element_type=F32
            )
            total = part if total is None else total + part
        for q in range(8):
            dx[q, :, cols] = total[q * 128 : q * 128 + 128].astype(BF16)

    for step in (2, 1):
        fill(step, 1)
        product(step, 1)
    start_far(1)
    fill(3, 1)
    product(3, 1)
    for step, dz in ((0, 1), (0, 0), (1, 0)):
        fill(step, dz)
    start_near(1)
    for step in (2, 3):
        fill(step, 0)
    for load in loads:
        load.wait()
    token_part(0)
    token_part(1)
    relay(1)
    token_part(2)

    first, last = pl.ds(0, 64), pl.ds(64, 64)
    columns = lambda y, zl: d_out.at[:, me.columns(y, zl)]
    l_in = {0: links.send(dx.at[me.block(2, 0), first, :], dl.at[0], up)}
    r_in = {0: links.send(dx.at[me.block(2, 0), last, :], dr.at[0], down)}
    z_in = {y: links.send(dx.at[me.block(y, 1)], zd.at[y], pair) for y in (2, 1, 3)}
    back = [
        links.send(dx.at[me.block(0, 1)], columns(0, 0), pair),
        links.send(dx.at[me.block(1, 0)], columns(0, 0), up),
        links.send(dx.at[me.block(3, 0)], columns(0, 0), down),
    ]
    keep = pltpu.make_async_copy(dx.at[me.b], columns(0, 0), own_sem)
    keep.start()

    def hand_on(dz):
        l_in[dz].wait_recv()
        back.append(links.send(dl.at[dz], d_out.at[first, me.columns(3, dz)], up))
        r_in[dz].wait_recv()
        back.append(links.send(dr.at[dz], d_out.at[last, me.columns(1, dz)], down))

    product(2, 0)
    product(1, 0)
    start_far(0)
    product(3, 0)
    z_in[2].wait_recv()
    l_in[1] = links.send(zd.at[2, first, :], dl.at[1], up)
    r_in[1] = links.send(zd.at[2, last, :], dr.at[1], down)
    hand_on(0)
    start_near(0)
    product(0, 1)
    z_in[1].wait_recv()
    back.append(links.send(zd.at[1], columns(0, 1), up))
    for group in (other_b, other_a, last_a, last_b):
        group[1].wait_recv()
    e = me.expert(0, 1)
    swapped[0, 1].wait_recv()
    add_rows(zs, [g.at[e, mine], cr.at[e], fl.at[1], fr.at[1]], 384)
    cross = links.send(zs, zr, far)
    z_in[3].wait_recv()
    back.append(links.send(zd.at[3], columns(0, 1), down))
    product(0, 0)
    hand_on(1)
    relay(0)
    for group in (other_b, other_a, last_a, last_b):
        group[0].wait_recv()
    swapped[0, 0].wait_recv()
    cross.wait_recv()
    e = me.expert(0, 0)
    add_rows(g_out, [g.at[e, mine], cr.at[e], fl.at[0], fr.at[0], zr], 384)
    gate_out[...] = g_out[:, :256]
    up_out[...] = g_out[:, 256:512]
    down_out[...] = jnp.transpose(g_out[:, 512:])
    for copy in back:
        copy.wait_recv()
    keep.wait()
    links.finish()


def finish(xt, ogt, ids, h, w):
    vmem, anywhere = pl.BlockSpec(memory_space=pltpu.VMEM), pl.BlockSpec(memory_space=pl.ANY)
    half, full = pltpu.VMEM((2, 192, 768), BF16), pltpu.VMEM((2, 384, 768), BF16)
    one = pltpu.VMEM((384, 768), BF16)
    return pl.pallas_call(
        finish_kernel,
        out_shape=(
            jax.ShapeDtypeStruct((128, 6144), BF16),
            jax.ShapeDtypeStruct((384, 256), F32),
            jax.ShapeDtypeStruct((384, 256), F32),
            jax.ShapeDtypeStruct((256, 384), F32),
        ),
        in_specs=[vmem] * 4 + [anywhere],
        out_specs=(anywhere,) + (vmem,) * 3,
        scratch_shapes=[
            pltpu.VMEM((8, 768, 768), BF16),
            pltpu.VMEM((8, 1024, 768), BF16),
            pltpu.VMEM((8, 2, 384, 768), BF16),
            pltpu.VMEM((8, 384, 768), BF16),
            pltpu.VMEM((8, 128, 768), BF16),
            pltpu.VMEM((384, 768), F32),
            pltpu.VMEM((4, 128, 768), BF16),
            pltpu.VMEM((2, 64, 768), BF16),
            pltpu.VMEM((2, 64, 768), BF16),
        ]
        + [full] + [half] * 6 + [full] * 2 + [one] * 2
        + [
            pltpu.SemaphoreType.DMA((FINISH_COPIES,)),
            pltpu.SemaphoreType.DMA((FINISH_COPIES,)),
            pltpu.SemaphoreType.DMA((8,)),
            pltpu.SemaphoreType.DMA,
        ],
        compiler_params=pltpu.CompilerParams(collective_id=2, has_side_effects=True, vmem_limit_bytes=60 << 20),
        name="finish",
    )(xt, ogt, ids, h, w)


def shards(tokens, out_grad, expert_ids, route_weight, w_gate, w_up, w_down):
    ids, weight = jnp.transpose(expert_ids), jnp.transpose(route_weight)
    h, xt, ogt, names, w = forward(tokens, out_grad, ids, weight, w_gate[0], w_up[0], w_down[0])
    d_tokens, gate, up, down = finish(xt, ogt, names, h, w.reshape(8, 768, 768))
    return d_tokens, gate[None], up[None], down[None]


def solution(mesh):
    in_specs = (
        P(("dp", "ep"), None),
        P(("dp", "ep"), None),
        P(("dp", "ep"), None),
        P(("dp", "ep"), None),
        P("ep", "dp", None),
        P("ep", "dp", None),
        P("ep", None, "dp"),
    )
    out_specs = (
        P(("dp", "ep"), None),
        P("ep", "dp", None),
        P("ep", "dp", None),
        P("ep", None, "dp"),
    )
    return jax.shard_map(shards, mesh=mesh, in_specs=in_specs, out_specs=out_specs, check_vma=False)
```

```python
import functools

import jax
import jax.numpy as jnp
from jax import lax
from jax.experimental import pallas as pl
from jax.experimental.pallas import tpu as pltpu
from jax.sharding import PartitionSpec as P

MESH = pl.DeviceIdType.MESH
F32, BF16 = jnp.float32, jnp.bfloat16
PEERS = [(dy, dz) for dy in (2, 1, 3, 0) for dz in (1, 0) if (dy, dz) != (0, 0)]


class Spot:
    def __init__(self):
        dp, ep = lax.axis_index("dp"), lax.axis_index("ep")
        self.y, self.zl, self.c = dp // 4, (dp // 2) % 2, dp % 2
        self.zh, self.x = ep // 4, ep % 4
        self.b = self.block(0, 0)

    def to(self, y=0, zl=0, c=0, zh=0, x=0):
        dp = (self.y + y) % 4 * 4 + (self.zl + zl) % 2 * 2 + (self.c + c) % 2
        return (dp, (self.zh + zh) % 2 * 4 + (self.x + x) % 4)

    def block(self, y, zl):
        return (self.zl + zl) % 2 * 4 + (self.y + y) % 4

    def columns(self, y, zl, width=768, offset=0):
        start = ((self.y + y) % 4 * 2 + (self.zl + zl) % 2) * 768 + offset
        return pl.ds(pl.multiple_of(start, 128), width)

    def expert(self, x, zh):
        return (self.zh + zh) % 2 * 4 + (self.x + x) % 4


class Links:
    def __init__(self, send_sem, recv_sem):
        self.send_sem, self.recv_sem, self.count, self.sent = send_sem, recv_sem, 0, []

    def send(self, src, dst, device):
        n = self.count
        self.count += 1
        copy = pltpu.make_async_remote_copy(
            src_ref=src,
            dst_ref=dst,
            send_sem=self.send_sem.at[n],
            recv_sem=self.recv_sem.at[n],
            device_id=device,
            device_id_type=MESH,
        )
        copy.start()
        self.sent.append(copy)
        return copy

    def finish(self):
        assert self.count == self.send_sem.shape[0]
        for copy in self.sent:
            copy.wait_send()


def greet(devices):
    barrier = pltpu.get_barrier_semaphore()
    for device in devices:
        pl.semaphore_signal(barrier, inc=1, device_id=device, device_id_type=MESH)
    pl.semaphore_wait(barrier, len(devices))


def add_rows(dst, sources, rows, step=32):
    @pl.loop(0, rows // step)
    def _(i):
        at = pl.ds(pl.multiple_of(i * step, step), step)
        total = sources[0][at, :].astype(F32)
        for source in sources[1:]:
            total = total + source[at, :].astype(F32)
        dst[at, :] = total.astype(dst.dtype)


def activation(pre, weight):
    gate, up, grad_hidden = pre[:, :256], pre[:, 256:512], pre[:, 512:] * weight
    sig = jax.nn.sigmoid(gate)
    silu = gate * sig
    hidden = silu * up * weight
    grad_gate = grad_hidden * up * sig * (1.0 + gate * (1.0 - sig))
    grad_up = grad_hidden * silu
    return grad_gate.astype(BF16), grad_up.astype(BF16), hidden.astype(BF16)


def open_sums(me, links, part, dz, sums):
    ra, rb, fl, fr = sums[2], sums[3], sums[6], sums[7]
    right, left = me.to(y=1), me.to(y=3)
    low, high = pl.ds(0, 64), pl.ds(64, 64)
    return (
        links.send(part.at[me.block(2, dz), low, :], ra.at[dz], right),
        links.send(part.at[me.block(2, dz), high, :], rb.at[dz], left),
        links.send(part.at[me.block(1, dz), high, :], fl.at[dz, high, :], right),
        links.send(part.at[me.block(3, dz), low, :], fr.at[dz, low, :], left),
    )


def close_sums(me, links, part, weight_rows, h_out, opened, sums, meanwhile):
    (
        weight8, weight, ra, rb, sa, sb, fl, fr, zs, zr, zin, s2, s1, s3, ra2, rb2, sa2, sb2, fl2, fr2, own, h_sem,
    ) = sums
    right, left, pair = me.to(y=1), me.to(y=3), me.to(zl=1)
    low, high = pl.ds(0, 64), pl.ds(64, 64)
    k0, k1, k1_low, k1_high = pl.ds(0, 128), pl.ds(128, 128), pl.ds(128, 64), pl.ds(192, 64)
    z_in = {2: links.send(part.at[me.block(2, 1), k1, :], zin.at[2], pair)}
    opened[1] = open_sums(me, links, part, 1, sums)
    first_a, first_b, other_b, other_a = [{dz: opened[dz][n] for dz in (0, 1)} for n in range(4)]
    last_a, last_b = {}, {}
    for y in (1, 3, 0):
        z_in[y] = links.send(part.at[me.block(y, 1), k1, :], zin.at[y], pair)
    weight8[...] = jnp.zeros((8, 128), F32)
    weight8[:2, :] = weight_rows[...]
    weight[...] = jnp.transpose(weight8[...])
    meanwhile()

    def relay(dz):
        first_a[dz].wait_recv()
        add_rows(sa.at[dz], [part.at[me.block(1, dz), low, :], ra.at[dz]], 64)
        last_a[dz] = links.send(sa.at[dz], fl.at[dz, low, :], right)
        first_b[dz].wait_recv()
        add_rows(sb.at[dz], [part.at[me.block(3, dz), high, :], rb.at[dz]], 64)
        last_b[dz] = links.send(sb.at[dz], fr.at[dz, high, :], left)

    relay(0)
    relay(1)
    z_in[2].wait_recv()
    add_rows(s2, [part.at[me.block(2, 0), k1, :], zin.at[2]], 128)
    far_a = links.send(s2.at[low, :], ra2, right)
    far_b = links.send(s2.at[high, :], rb2, left)
    z_in[1].wait_recv()
    add_rows(s1, [part.at[me.block(1, 0), k1_high, :], zin.at[1, high, :]], 64)
    side_b = links.send(s1, fl2.at[high, :], right)
    for group in (other_b, other_a, last_a, last_b):
        group[1].wait_recv()
    add_rows(zs, [part.at[me.block(0, 1), k0, :], fl.at[1], fr.at[1]], 128)
    cross = links.send(zs, zr, pair)
    z_in[3].wait_recv()
    add_rows(s3, [part.at[me.block(3, 0), k1_low, :], zin.at[3, low, :]], 64)
    side_a = links.send(s3, fr2.at[low, :], left)
    far_a.wait_recv()
    add_rows(sa2, [part.at[me.block(1, 0), k1_low, :], zin.at[1, low, :], ra2], 64)
    end_a = links.send(sa2, fl2.at[low, :], right)
    far_b.wait_recv()
    add_rows(sb2, [part.at[me.block(3, 0), k1_high, :], zin.at[3, high, :], rb2], 64)
    end_b = links.send(sb2, fr2.at[high, :], left)

    def active(k, sources):
        @pl.loop(0, 8)
        def _(i):
            row = pl.multiple_of(i * 16, 16)
            at = pl.ds(k * 128 + row, 16)
            pre = part[me.b, at, :].astype(F32)
            for source in sources:
                pre = pre + source[pl.ds(row, 16), :].astype(F32)
            own[at, :256], own[at, 256:512], own[at, 512:] = activation(pre, weight[pl.ds(row, 16), k : k + 1])

    for group in (other_b, other_a, last_a, last_b):
        group[0].wait_recv()
    cross.wait_recv()
    active(0, [fl.at[0], fr.at[0], zr])
    mine0 = pltpu.make_async_copy(own.at[k0, :], h_out.at[me.b, k0, :], h_sem.at[0])
    mine0.start()
    from_pair = links.send(own.at[k0, :], h_out.at[me.b, k0, :], pair)
    from_left = {0: links.send(own.at[k0, :], h_out.at[me.b, k0, :], right)}
    from_right = {0: links.send(own.at[k0, :], h_out.at[me.b, k0, :], left)}

    def pass_on(block, device, rows):
        piece = h_out.at[block, rows, :]
        return links.send(piece, piece, device)

    for copy in (z_in[0], side_a, side_b, end_a, end_b):
        copy.wait_recv()
    active(1, [zin.at[0], fl2, fr2])
    mine1 = pltpu.make_async_copy(own.at[k1, :], h_out.at[me.b, k1, :], h_sem.at[1])
    mine1.start()
    left1 = links.send(own.at[k1, :], h_out.at[me.b, k1, :], right)
    right1 = links.send(own.at[k1, :], h_out.at[me.b, k1, :], left)
    tail = [links.send(own.at[k1, :], h_out.at[me.b, k1, :], pair)]
    from_pair.wait_recv()
    from_left[1] = pass_on(me.block(0, 1), right, k0)
    from_right[1] = pass_on(me.block(0, 1), left, k0)
    from_left[0].wait_recv()
    tail.append(pass_on(me.block(3, 0), right, low))
    from_right[0].wait_recv()
    tail.append(pass_on(me.block(1, 0), left, high))
    left1.wait_recv()
    half_a = pass_on(me.block(3, 0), right, k1_low)
    tail.append(pass_on(me.block(3, 0), pair, k1))
    right1.wait_recv()
    half_b = pass_on(me.block(1, 0), left, k1_high)
    tail.append(pass_on(me.block(1, 0), pair, k1))
    from_left[1].wait_recv()
    tail.append(pass_on(me.block(3, 1), right, low))
    from_right[1].wait_recv()
    tail.append(pass_on(me.block(1, 1), left, high))
    half_a.wait_recv()
    half_b.wait_recv()
    tail.append(pass_on(me.block(2, 0), pair, k1))
    for copy in tail:
        copy.wait_recv()
    mine0.wait()
    mine1.wait()


FORWARD_COPIES = 19 + 24 + 7 + 40


def forward_kernel(
    tok, og, ids_rows, weight_rows, gate_in, up_in, down_in, h_out, xt, ogt, idc, w_out,
    part, w_in, ids, x, g, ids_in, w, z_tok, z_og, l_tok, r_og, send_sem, recv_sem, own_sem, w_sem, *sums
):
    me = Spot()
    right, left, up, down = me.to(x=1), me.to(x=3), me.to(y=1), me.to(y=3)
    core, far, pair = me.to(c=1), me.to(zh=1), me.to(zl=1)
    w_in[:, :256] = gate_in[...]
    w_in[:, 256:512] = up_in[...]
    w_in[:, 512:] = jnp.transpose(down_in[...])
    ids[...] = jnp.zeros((8, 128), jnp.int32)
    ids[:2, :] = ids_rows[...]
    greet([me.to(y=dy, zl=dz) for dy, dz in PEERS] + [right, left, core, far])
    links = Links(send_sem, recv_sem)
    own, far_e = me.expert(0, 0), me.expert(0, 1)

    from_far = links.send(w_in, w.at[own, me.c], far)
    from_left0 = links.send(w_in, w.at[own, me.c], right)
    from_right0 = links.send(w_in, w.at[own, me.c], left)
    from_core = {(0, 0): [links.send(w_in, w.at[own, me.c], core)]}

    def cut(array, y, zl):
        return array.at[:, me.columns(y, zl)]

    plane = [
        links.send(cut(tok, 2, 0), l_tok.at[0], up),
        links.send(cut(og, 2, 0), r_og.at[0], down),
    ]
    z_in = {}
    z_in[2, 0] = links.send(cut(tok, 2, 1), z_tok.at[2], pair)
    z_in[2, 1] = links.send(cut(og, 2, 1), z_og.at[2], pair)
    near = []
    for y, device in ((1, up), (3, down)):
        near.append(links.send(cut(tok, y, 0), x.at[me.b], device))
        near.append(links.send(cut(og, y, 0), g.at[me.b], device))
    for y in (1, 3):
        z_in[y, 0] = links.send(cut(tok, y, 1), z_tok.at[y], pair)
        z_in[y, 1] = links.send(cut(og, y, 1), z_og.at[y], pair)
    z_in[0, 0] = links.send(cut(tok, 0, 1), x.at[me.b], pair)
    z_in[0, 1] = links.send(cut(og, 0, 1), g.at[me.b], pair)
    names = [links.send(ids, ids_in.at[me.b], me.to(y=dy, zl=dz)) for dy, dz in PEERS]
    local = [
        pltpu.make_async_copy(w_in, w.at[own, me.c], own_sem.at[0]),
        pltpu.make_async_copy(cut(tok, 0, 0), x.at[me.b], own_sem.at[1]),
        pltpu.make_async_copy(cut(og, 0, 0), g.at[me.b], own_sem.at[2]),
        pltpu.make_async_copy(ids, ids_in.at[me.b], own_sem.at[3]),
    ]
    for copy in local:
        copy.start()

    @pl.loop(0, 64)
    def _(i):
        part[i // 8, pl.ds(pl.multiple_of(i % 8 * 32, 32), 32), :] = jnp.zeros((32, 768), BF16)

    def pass_on(expert, device, rows=pl.ds(0, 384)):
        piece = w.at[expert, me.c, rows, :]
        return links.send(piece, piece, device)

    low, high = pl.ds(0, 192), pl.ds(192, 192)
    across, ends = [], []
    z_in[2, 0].wait_recv()
    across.append(links.send(z_tok.at[2], l_tok.at[1], up))
    plane[0].wait_recv()
    ends.append(links.send(l_tok.at[0], x.at[me.block(3, 0)], up))
    z_in[2, 1].wait_recv()
    across.append(links.send(z_og.at[2], r_og.at[1], down))
    plane[1].wait_recv()
    ends.append(links.send(r_og.at[0], g.at[me.block(1, 0)], down))
    halves = {0: [], 1: []}

    def sideways(dz, from_left, from_right):
        from_left.wait_recv()
        halves[dz].append(pass_on(me.expert(3, dz), right, low))
        from_core[3, dz] = [pass_on(me.expert(3, dz), core)]
        from_right.wait_recv()
        halves[dz].append(pass_on(me.expert(1, dz), left, high))
        from_core[1, dz] = [pass_on(me.expert(1, dz), core)]

    sideways(0, from_left0, from_right0)
    late = []

    def partner(y, device):
        z_in[y, 0].wait_recv()
        late.append(links.send(z_tok.at[y], x.at[me.block(0, 1)], device))
        z_in[y, 1].wait_recv()
        late.append(links.send(z_og.at[y], g.at[me.block(0, 1)], device))

    from_far.wait_recv()
    from_left1 = pass_on(far_e, right)
    from_right1 = pass_on(far_e, left)
    from_core[0, 1] = [pass_on(far_e, core)]
    partner(1, up)
    partner(3, down)
    across[0].wait_recv()
    late.append(links.send(l_tok.at[1], x.at[me.block(3, 1)], up))
    across[1].wait_recv()
    late.append(links.send(r_og.at[1], g.at[me.block(1, 1)], down))

    def second(dz):
        from_core[2, dz] = []
        for n, half in enumerate(halves[dz]):
            half.wait_recv()
            from_core[2, dz].append(pass_on(me.expert(2, dz), core, (low, high)[n]))

    def turn(dz):
        for y in range(4):
            b = me.block(y, dz)
            at = pl.ds(pl.multiple_of(b * 128, 128), 128)
            xt[:, at] = jnp.transpose(x[b])
            ogt[:, at] = jnp.transpose(g[b])

    def name_rows(dz):
        for y in range(4):
            b = me.block(y, dz)
            at = pl.ds(pl.multiple_of(b * 128, 128), 128)
            idc[at, :] = jnp.transpose(ids_in[b])

    def keep(step, dz):
        for copy in from_core[step, dz]:
            copy.wait_recv()
        e = me.expert(step, dz)
        pltpu.make_async_copy(w.at[e], w_out.at[e], w_sem.at[e]).start()

    def product(e, dz):
        plane_at = pl.multiple_of((me.zl + dz) % 2 * 4, 4)
        for n, source in ((0, x), (1, x), (2, g)):
            cols = slice(n * 256, n * 256 + 256)
            rows = source[pl.ds(plane_at, 4)].reshape(512, 768)
            out = jnp.dot(rows, w[e, :, :, cols].reshape(768, 256), preferred_element_type=F32)
            for y in range(4):
                names_at = pl.ds(pl.multiple_of((plane_at + y) * 128, 128), 128)
                for k in range(2):
                    here = part.at[plane_at + y, k * 128 : k * 128 + 128, cols]
                    chosen = idc[names_at, k : k + 1] == e
                    old = here[...].astype(F32)
                    here[...] = jnp.where(chosen, out[y * 128 : y * 128 + 128], old).astype(BF16)

    def first_six(i):
        g2 = i // 2
        step = (g2 + 1) // 2 * (1 + 2 * (i % 2))
        return me.expert(step, (1 - (g2 + 1) // 2) * (i % 2) + g2 // 2)

    for copy in near + ends + names:
        copy.wait_recv()
    for copy in local:
        copy.wait()
    turn(0)
    name_rows(0)
    for step, dz in ((0, 0), (0, 1), (1, 0), (3, 0)):
        keep(step, dz)

    @pl.loop(0, 4)
    def _(i):
        product(first_six(i), 0)

    second(0)
    sideways(1, from_left1, from_right1)
    keep(1, 1)
    keep(3, 1)

    @pl.loop(4, 6)
    def _(i):
        product(first_six(i), 0)

    for copy in [z_in[0, 0], z_in[0, 1]] + late:
        copy.wait_recv()
    name_rows(1)

    @pl.loop(0, 6)
    def _(i):
        product(first_six(i), 1)

    second(1)
    keep(2, 0)
    keep(2, 1)

    @pl.loop(0, 2)
    def _(i):
        product(me.expert(2, i), 0)

    opened = {0: open_sums(me, links, part, 0, sums)}

    @pl.loop(0, 2)
    def _(i):
        product(me.expert(2, i), 1)

    close_sums(me, links, part, weight_rows, h_out, opened, sums, lambda: turn(1))
    links.finish()
    for e in range(8):
        pltpu.make_async_copy(w.at[e], w_out.at[e], w_sem.at[e]).wait()


def forward(tokens, out_grad, ids, weight, w_gate, w_up, w_down):
    vmem, anywhere = pl.BlockSpec(memory_space=pltpu.VMEM), pl.BlockSpec(memory_space=pl.ANY)
    blocks = lambda n: pltpu.VMEM((n, 128, 768), BF16)
    rows = lambda *shape: pltpu.VMEM(shape + (768,), BF16)
    return pl.pallas_call(
        forward_kernel,
        out_shape=(
            jax.ShapeDtypeStruct((8, 256, 768), BF16),
            jax.ShapeDtypeStruct((768, 1024), BF16),
            jax.ShapeDtypeStruct((768, 1024), BF16),
            jax.ShapeDtypeStruct((1024, 8), jnp.int32),
            jax.ShapeDtypeStruct((8, 2, 384, 768), BF16),
        ),
        in_specs=[vmem] * 7,
        out_specs=(anywhere,) + (vmem,) * 3 + (anywhere,),
        scratch_shapes=[
            pltpu.VMEM((8, 256, 768), BF16),
            pltpu.VMEM((384, 768), BF16),
            pltpu.VMEM((8, 128), jnp.int32),
            blocks(8),
            blocks(8),
            pltpu.VMEM((8, 8, 128), jnp.int32),
            pltpu.VMEM((8, 2, 384, 768), BF16),
            blocks(4),
            blocks(4),
            blocks(2),
            blocks(2),
            pltpu.SemaphoreType.DMA((FORWARD_COPIES,)),
            pltpu.SemaphoreType.DMA((FORWARD_COPIES,)),
            pltpu.SemaphoreType.DMA((4,)),
            pltpu.SemaphoreType.DMA((8,)),
            pltpu.VMEM((8, 128), F32),
            pltpu.VMEM((128, 8), F32),
        ]
        + [rows(2, 64)] * 4
        + [rows(2, 128)] * 2
        + [rows(128)] * 2
        + [rows(4, 128), rows(128)]
        + [rows(64)] * 6
        + [rows(128)] * 2
        + [rows(256), pltpu.SemaphoreType.DMA((2,))],
        compiler_params=pltpu.CompilerParams(collective_id=0, has_side_effects=True, vmem_limit_bytes=60 << 20),
        name="forward",
    )(tokens, out_grad, ids, weight, w_gate, w_up, w_down)


FINISH_COPIES = 8 + 4 + 4 + 4 + 1 + 16


def finish_kernel(
    xt_in, ogt_in, ids_in, h_in, w, d_out, gate_out, up_out, down_out,
    xt, ogt, ids, h, w_all, he, g, cr, dx, g_out, zd, dl, dr, a2, ra, rb, sa, sb, oa, ob, fl, fr, zs, zr,
    send_sem, recv_sem, w_sem, own_sem,
):
    me = Spot()
    right, left, core, far = me.to(x=1), me.to(x=3), me.to(c=1), me.to(zh=1)
    up, down, pair = me.to(y=1), me.to(y=3), me.to(zl=1)
    sources = ((ids_in, ids), (h_in, h), (xt_in, xt), (ogt_in, ogt))
    heads = [pltpu.make_async_copy(src, dst, w_sem.at[8 + n]) for n, (src, dst) in enumerate(sources)]
    loads = [pltpu.make_async_copy(w.at[e], w_all.at[e], w_sem.at[e]) for e in range(8)]
    for load in heads + loads:
        load.start()
    greet([up, down, pair, right, left, core, far])
    links = Links(send_sem, recv_sem)
    low, high = pl.ds(0, 192), pl.ds(192, 192)
    mine, others = me.c, 1 - me.c
    swapped, first_a, first_b, other_b, other_a, last_a, last_b = {}, {}, {}, {}, {}, {}, {}

    def fill(step, dz):
        e = me.expert(step, dz)

        @pl.loop(0, 8)
        def _(q):
            at = pl.ds(pl.multiple_of(q * 128, 128), 128)
            chosen = [(ids[at, k : k + 1] == e).astype(F32) for k in range(2)]
            m0, m1 = [jnp.broadcast_to(m, (128, 128)).astype(BF16) for m in chosen]
            for n in range(6):
                cols = slice(n * 128, n * 128 + 128)
                he[e, at, cols] = h[q, :128, cols] * m0 + h[q, 128:, cols] * m1

    def product(step, dz):
        e = me.expert(step, dz)
        for n, left_t in ((0, xt), (1, xt), (2, ogt)):
            cols = slice(n * 256, n * 256 + 256)
            out = jnp.dot(left_t[...], he[e, :, cols], preferred_element_type=F32).astype(BF16)
            g[e, 0, :, cols] = out[:384]
            g[e, 1, :, cols] = out[384:]
        swapped[step, dz] = links.send(g.at[e, others], cr.at[e], core)

    def start_far(dz):
        e = me.expert(2, dz)
        swapped[2, dz].wait_recv()
        add_rows(a2.at[dz], [g.at[e, mine], cr.at[e]], 384)
        first_a[dz] = links.send(a2.at[dz, low, :], ra.at[dz], right)
        first_b[dz] = links.send(a2.at[dz, high, :], rb.at[dz], left)

    def start_near(dz):
        e = me.expert(1, dz)
        swapped[1, dz].wait_recv()
        add_rows(ob.at[dz], [g.at[e, mine, high, :], cr.at[e, high, :]], 192)
        other_b[dz] = links.send(ob.at[dz], fl.at[dz, high, :], right)
        e = me.expert(3, dz)
        swapped[3, dz].wait_recv()
        add_rows(oa.at[dz], [g.at[e, mine, low, :], cr.at[e, low, :]], 192)
        other_a[dz] = links.send(oa.at[dz], fr.at[dz, low, :], left)

    def relay(dz):
        e = me.expert(1, dz)
        first_a[dz].wait_recv()
        add_rows(sa.at[dz], [g.at[e, mine, low, :], cr.at[e, low, :], ra.at[dz]], 192)
        last_a[dz] = links.send(sa.at[dz], fl.at[dz, low, :], right)
        e = me.expert(3, dz)
        first_b[dz].wait_recv()
        add_rows(sb.at[dz], [g.at[e, mine, high, :], cr.at[e, high, :], rb.at[dz]], 192)
        last_b[dz] = links.send(sb.at[dz], fr.at[dz, high, :], left)

    def token_part(n):
        cols = slice(n * 256, n * 256 + 256)
        total = None
        for e in range(8):
            part = lax.dot_general(
                he[e, :, :512], w_all[e, cols, :512], (((1,), (1,)), ((), ())), preferred_element_type=F32
            )
            total = part if total is None else total + part
        for q in range(8):
            dx[q, :, cols] = total[q * 128 : q * 128 + 128].astype(BF16)

    for load in heads:
        load.wait()
    for step in (2, 1):
        fill(step, 1)
        product(step, 1)
    start_far(1)
    fill(3, 1)
    product(3, 1)
    for step, dz in ((0, 1), (0, 0), (1, 0)):
        fill(step, dz)
    start_near(1)
    for step in (2, 3):
        fill(step, 0)
    for load in loads:
        load.wait()
    token_part(0)
    token_part(1)
    relay(1)
    token_part(2)

    first, last = pl.ds(0, 64), pl.ds(64, 64)
    columns = lambda y, zl: d_out.at[:, me.columns(y, zl)]
    l_in = {0: links.send(dx.at[me.block(2, 0), first, :], dl.at[0], up)}
    r_in = {0: links.send(dx.at[me.block(2, 0), last, :], dr.at[0], down)}
    z_in = {y: links.send(dx.at[me.block(y, 1)], zd.at[y], pair) for y in (2, 1, 3)}
    back = [
        links.send(dx.at[me.block(0, 1)], columns(0, 0), pair),
        links.send(dx.at[me.block(1, 0)], columns(0, 0), up),
        links.send(dx.at[me.block(3, 0)], columns(0, 0), down),
    ]
    keep = pltpu.make_async_copy(dx.at[me.b], columns(0, 0), own_sem)
    keep.start()

    def hand_on(dz):
        l_in[dz].wait_recv()
        back.append(links.send(dl.at[dz], d_out.at[first, me.columns(3, dz)], up))
        r_in[dz].wait_recv()
        back.append(links.send(dr.at[dz], d_out.at[last, me.columns(1, dz)], down))

    product(2, 0)
    product(1, 0)
    start_far(0)
    product(3, 0)
    z_in[2].wait_recv()
    l_in[1] = links.send(zd.at[2, first, :], dl.at[1], up)
    r_in[1] = links.send(zd.at[2, last, :], dr.at[1], down)
    hand_on(0)
    start_near(0)
    product(0, 1)
    z_in[1].wait_recv()
    back.append(links.send(zd.at[1], columns(0, 1), up))
    for group in (other_b, other_a, last_a, last_b):
        group[1].wait_recv()
    e = me.expert(0, 1)
    swapped[0, 1].wait_recv()
    add_rows(zs, [g.at[e, mine], cr.at[e], fl.at[1], fr.at[1]], 384)
    cross = links.send(zs, zr, far)
    z_in[3].wait_recv()
    back.append(links.send(zd.at[3], columns(0, 1), down))
    product(0, 0)
    hand_on(1)
    relay(0)
    for group in (other_b, other_a, last_a, last_b):
        group[0].wait_recv()
    swapped[0, 0].wait_recv()
    cross.wait_recv()
    e = me.expert(0, 0)
    add_rows(g_out, [g.at[e, mine], cr.at[e], fl.at[0], fr.at[0], zr], 384)
    gate_out[...] = g_out[:, :256]
    up_out[...] = g_out[:, 256:512]
    down_out[...] = jnp.transpose(g_out[:, 512:])
    for copy in back:
        copy.wait_recv()
    keep.wait()
    links.finish()


def finish(xt, ogt, ids, h, w):
    vmem, anywhere = pl.BlockSpec(memory_space=pltpu.VMEM), pl.BlockSpec(memory_space=pl.ANY)
    half, full = pltpu.VMEM((2, 192, 768), BF16), pltpu.VMEM((2, 384, 768), BF16)
    one = pltpu.VMEM((384, 768), BF16)
    return pl.pallas_call(
        finish_kernel,
        out_shape=(
            jax.ShapeDtypeStruct((128, 6144), BF16),
            jax.ShapeDtypeStruct((384, 256), F32),
            jax.ShapeDtypeStruct((384, 256), F32),
            jax.ShapeDtypeStruct((256, 384), F32),
        ),
        in_specs=[anywhere] * 5,
        out_specs=(anywhere,) + (vmem,) * 3,
        scratch_shapes=[
            pltpu.VMEM((768, 1024), BF16),
            pltpu.VMEM((768, 1024), BF16),
            pltpu.VMEM((1024, 8), jnp.int32),
            pltpu.VMEM((8, 256, 768), BF16),
            pltpu.VMEM((8, 768, 768), BF16),
            pltpu.VMEM((8, 1024, 768), BF16),
            pltpu.VMEM((8, 2, 384, 768), BF16),
            pltpu.VMEM((8, 384, 768), BF16),
            pltpu.VMEM((8, 128, 768), BF16),
            pltpu.VMEM((384, 768), F32),
            pltpu.VMEM((4, 128, 768), BF16),
            pltpu.VMEM((2, 64, 768), BF16),
            pltpu.VMEM((2, 64, 768), BF16),
        ]
        + [full] + [half] * 6 + [full] * 2 + [one] * 2
        + [
            pltpu.SemaphoreType.DMA((FINISH_COPIES,)),
            pltpu.SemaphoreType.DMA((FINISH_COPIES,)),
            pltpu.SemaphoreType.DMA((12,)),
            pltpu.SemaphoreType.DMA,
        ],
        compiler_params=pltpu.CompilerParams(collective_id=2, has_side_effects=True, vmem_limit_bytes=60 << 20),
        name="finish",
    )(xt, ogt, ids, h, w)


def deliver_kernel(*refs):
    sources, results, places = refs[:4], refs[4:8], refs[8:12]
    in_sem, out_sem = refs[12:]
    pieces = []
    for n in range(4):
        rows = sources[n].shape[0]
        step = 32 if n == 0 else rows
        for row in range(0, rows, step):
            pieces.append((n, pl.ds(row, step)))
    fetch = [pltpu.make_async_copy(sources[n].at[at], places[n].at[at], in_sem.at[i]) for i, (n, at) in enumerate(pieces)]
    store = [pltpu.make_async_copy(places[n].at[at], results[n].at[at], out_sem.at[i]) for i, (n, at) in enumerate(pieces)]
    for copy in fetch:
        copy.start()
    for first, second in zip(fetch, store):
        first.wait()
        second.start()
    for copy in store:
        copy.wait()


def deliver(*arrays):
    anywhere = pl.BlockSpec(memory_space=pl.ANY)
    return pl.pallas_call(
        deliver_kernel,
        out_shape=tuple(jax.ShapeDtypeStruct(a.shape, a.dtype) for a in arrays),
        in_specs=[anywhere] * 4,
        out_specs=(anywhere,) * 4,
        scratch_shapes=[pltpu.VMEM(a.shape, a.dtype) for a in arrays]
        + [pltpu.SemaphoreType.DMA((7,)), pltpu.SemaphoreType.DMA((7,))],
        name="deliver",
    )(*arrays)


def shards(tokens, out_grad, expert_ids, route_weight, w_gate, w_up, w_down):
    ids, weight = jnp.transpose(expert_ids), jnp.transpose(route_weight)
    h, xt, ogt, names, w = forward(tokens, out_grad, ids, weight, w_gate[0], w_up[0], w_down[0])
    d_tokens, gate, up, down = deliver(*finish(xt, ogt, names, h, w.reshape(8, 768, 768)))
    return d_tokens, gate[None], up[None], down[None]


def solution(mesh):
    in_specs = (
        P(("dp", "ep"), None),
        P(("dp", "ep"), None),
        P(("dp", "ep"), None),
        P(("dp", "ep"), None),
        P("ep", "dp", None),
        P("ep", "dp", None),
        P("ep", None, "dp"),
    )
    out_specs = (
        P(("dp", "ep"), None),
        P("ep", "dp", None),
        P("ep", "dp", None),
        P("ep", None, "dp"),
    )
    return jax.shard_map(shards, mesh=mesh, in_specs=in_specs, out_specs=out_specs, check_vma=False)
```

```python
import functools

import jax
import jax.numpy as jnp
from jax import lax
from jax.experimental import pallas as pl
from jax.experimental.pallas import tpu as pltpu
from jax.sharding import PartitionSpec as P

MESH = pl.DeviceIdType.MESH
F32, BF16 = jnp.float32, jnp.bfloat16
PEERS = [(dy, dz) for dy in (2, 1, 3, 0) for dz in (1, 0) if (dy, dz) != (0, 0)]


class Spot:
    def __init__(self):
        dp, ep = lax.axis_index("dp"), lax.axis_index("ep")
        self.y, self.zl, self.c = dp // 4, (dp // 2) % 2, dp % 2
        self.zh, self.x = ep // 4, ep % 4
        self.b = self.block(0, 0)

    def to(self, y=0, zl=0, c=0, zh=0, x=0):
        dp = (self.y + y) % 4 * 4 + (self.zl + zl) % 2 * 2 + (self.c + c) % 2
        return (dp, (self.zh + zh) % 2 * 4 + (self.x + x) % 4)

    def block(self, y, zl):
        return (self.zl + zl) % 2 * 4 + (self.y + y) % 4

    def columns(self, y, zl, width=768, offset=0):
        start = ((self.y + y) % 4 * 2 + (self.zl + zl) % 2) * 768 + offset
        return pl.ds(pl.multiple_of(start, 128), width)

    def expert(self, x, zh):
        return (self.zh + zh) % 2 * 4 + (self.x + x) % 4


class Links:
    def __init__(self, send_sem, recv_sem):
        self.send_sem, self.recv_sem, self.count, self.sent = send_sem, recv_sem, 0, []

    def send(self, src, dst, device):
        n = self.count
        self.count += 1
        copy = pltpu.make_async_remote_copy(
            src_ref=src,
            dst_ref=dst,
            send_sem=self.send_sem.at[n],
            recv_sem=self.recv_sem.at[n],
            device_id=device,
            device_id_type=MESH,
        )
        copy.start()
        self.sent.append(copy)
        return copy

    def finish(self):
        assert self.count == self.send_sem.shape[0]
        for copy in self.sent:
            copy.wait_send()


def greet(devices):
    barrier = pltpu.get_barrier_semaphore()
    for device in devices:
        pl.semaphore_signal(barrier, inc=1, device_id=device, device_id_type=MESH)
    pl.semaphore_wait(barrier, len(devices))


def add_rows(dst, sources, rows, step=32):
    @pl.loop(0, rows // step)
    def _(i):
        at = pl.ds(pl.multiple_of(i * step, step), step)
        total = sources[0][at, :].astype(F32)
        for source in sources[1:]:
            total = total + source[at, :].astype(F32)
        dst[at, :] = total.astype(dst.dtype)


def activation(pre, weight):
    gate, up, grad_hidden = pre[:, :256], pre[:, 256:512], pre[:, 512:] * weight
    sig = jax.nn.sigmoid(gate)
    silu = gate * sig
    hidden = silu * up * weight
    grad_gate = grad_hidden * up * sig * (1.0 + gate * (1.0 - sig))
    grad_up = grad_hidden * silu
    return grad_gate.astype(BF16), grad_up.astype(BF16), hidden.astype(BF16)


def open_sums(me, links, part, dz, sums):
    ra, rb, fl, fr = sums[2], sums[3], sums[6], sums[7]
    right, left = me.to(y=1), me.to(y=3)
    low, high = pl.ds(0, 64), pl.ds(64, 64)
    return (
        links.send(part.at[me.block(2, dz), low, :], ra.at[dz], right),
        links.send(part.at[me.block(2, dz), high, :], rb.at[dz], left),
        links.send(part.at[me.block(1, dz), high, :], fl.at[dz, high, :], right),
        links.send(part.at[me.block(3, dz), low, :], fr.at[dz, low, :], left),
    )


def close_sums(me, links, part, weight_rows, h_out, opened, sums, meanwhile):
    (
        weight8, weight, ra, rb, sa, sb, fl, fr, zs, zr, zin, s2, s1, s3, ra2, rb2, sa2, sb2, fl2, fr2, own, h_sem,
    ) = sums
    right, left, pair = me.to(y=1), me.to(y=3), me.to(zl=1)
    low, high = pl.ds(0, 64), pl.ds(64, 64)
    k0, k1, k1_low, k1_high = pl.ds(0, 128), pl.ds(128, 128), pl.ds(128, 64), pl.ds(192, 64)
    z_in = {2: links.send(part.at[me.block(2, 1), k1, :], zin.at[2], pair)}
    opened[1] = open_sums(me, links, part, 1, sums)
    first_a, first_b, other_b, other_a = [{dz: opened[dz][n] for dz in (0, 1)} for n in range(4)]
    last_a, last_b = {}, {}
    for y in (1, 3, 0):
        z_in[y] = links.send(part.at[me.block(y, 1), k1, :], zin.at[y], pair)
    weight8[...] = jnp.zeros((8, 128), F32)
    weight8[:2, :] = weight_rows[...]
    weight[...] = jnp.transpose(weight8[...])

    def relay(dz):
        first_a[dz].wait_recv()
        add_rows(sa.at[dz], [part.at[me.block(1, dz), low, :], ra.at[dz]], 64)
        last_a[dz] = links.send(sa.at[dz], fl.at[dz, low, :], right)
        first_b[dz].wait_recv()
        add_rows(sb.at[dz], [part.at[me.block(3, dz), high, :], rb.at[dz]], 64)
        last_b[dz] = links.send(sb.at[dz], fr.at[dz, high, :], left)

    relay(0)
    meanwhile()
    relay(1)
    z_in[2].wait_recv()
    add_rows(s2, [part.at[me.block(2, 0), k1, :], zin.at[2]], 128)
    far_a = links.send(s2.at[low, :], ra2, right)
    far_b = links.send(s2.at[high, :], rb2, left)
    z_in[1].wait_recv()
    add_rows(s1, [part.at[me.block(1, 0), k1_high, :], zin.at[1, high, :]], 64)
    side_b = links.send(s1, fl2.at[high, :], right)
    for group in (other_b, other_a, last_a, last_b):
        group[1].wait_recv()
    add_rows(zs, [part.at[me.block(0, 1), k0, :], fl.at[1], fr.at[1]], 128)
    cross = links.send(zs, zr, pair)
    z_in[3].wait_recv()
    add_rows(s3, [part.at[me.block(3, 0), k1_low, :], zin.at[3, low, :]], 64)
    side_a = links.send(s3, fr2.at[low, :], left)
    far_a.wait_recv()
    add_rows(sa2, [part.at[me.block(1, 0), k1_low, :], zin.at[1, low, :], ra2], 64)
    end_a = links.send(sa2, fl2.at[low, :], right)
    far_b.wait_recv()
    add_rows(sb2, [part.at[me.block(3, 0), k1_high, :], zin.at[3, high, :], rb2], 64)
    end_b = links.send(sb2, fr2.at[high, :], left)

    def active(k, sources):
        @pl.loop(0, 8)
        def _(i):
            row = pl.multiple_of(i * 16, 16)
            at = pl.ds(k * 128 + row, 16)
            pre = part[me.b, at, :].astype(F32)
            for source in sources:
                pre = pre + source[pl.ds(row, 16), :].astype(F32)
            own[at, :256], own[at, 256:512], own[at, 512:] = activation(pre, weight[pl.ds(row, 16), k : k + 1])

    for group in (other_b, other_a, last_a, last_b):
        group[0].wait_recv()
    cross.wait_recv()
    active(0, [fl.at[0], fr.at[0], zr])
    mine0 = pltpu.make_async_copy(own.at[k0, :], h_out.at[me.b, k0, :], h_sem.at[0])
    mine0.start()
    from_pair = links.send(own.at[k0, :], h_out.at[me.b, k0, :], pair)
    from_left = {0: links.send(own.at[k0, :], h_out.at[me.b, k0, :], right)}
    from_right = {0: links.send(own.at[k0, :], h_out.at[me.b, k0, :], left)}

    def pass_on(block, device, rows):
        piece = h_out.at[block, rows, :]
        return links.send(piece, piece, device)

    for copy in (z_in[0], side_a, side_b, end_a, end_b):
        copy.wait_recv()
    active(1, [zin.at[0], fl2, fr2])
    mine1 = pltpu.make_async_copy(own.at[k1, :], h_out.at[me.b, k1, :], h_sem.at[1])
    mine1.start()
    left1 = links.send(own.at[k1, :], h_out.at[me.b, k1, :], right)
    right1 = links.send(own.at[k1, :], h_out.at[me.b, k1, :], left)
    tail = [links.send(own.at[k1, :], h_out.at[me.b, k1, :], pair)]
    from_pair.wait_recv()
    from_left[1] = pass_on(me.block(0, 1), right, k0)
    from_right[1] = pass_on(me.block(0, 1), left, k0)
    from_left[0].wait_recv()
    tail.append(pass_on(me.block(3, 0), right, low))
    from_right[0].wait_recv()
    tail.append(pass_on(me.block(1, 0), left, high))
    left1.wait_recv()
    half_a = pass_on(me.block(3, 0), right, k1_low)
    tail.append(pass_on(me.block(3, 0), pair, k1))
    right1.wait_recv()
    half_b = pass_on(me.block(1, 0), left, k1_high)
    tail.append(pass_on(me.block(1, 0), pair, k1))
    from_left[1].wait_recv()
    tail.append(pass_on(me.block(3, 1), right, low))
    from_right[1].wait_recv()
    tail.append(pass_on(me.block(1, 1), left, high))
    half_a.wait_recv()
    half_b.wait_recv()
    tail.append(pass_on(me.block(2, 0), pair, k1))
    for copy in tail:
        copy.wait_recv()
    mine0.wait()
    mine1.wait()


FORWARD_COPIES = 19 + 24 + 7 + 40


def forward_kernel(
    tok, og, ids_rows, weight_rows, gate_in, up_in, down_in, h_out, xt, ogt, idc, w_out,
    part, w_in, ids, x, g, ids_in, w, z_tok, z_og, l_tok, r_og, send_sem, recv_sem, own_sem, w_sem, *sums
):
    me = Spot()
    right, left, up, down = me.to(x=1), me.to(x=3), me.to(y=1), me.to(y=3)
    core, far, pair = me.to(c=1), me.to(zh=1), me.to(zl=1)
    w_in[:, :256] = gate_in[...]
    w_in[:, 256:512] = up_in[...]
    w_in[:, 512:] = jnp.transpose(down_in[...])
    ids[...] = jnp.zeros((8, 128), jnp.int32)
    ids[:2, :] = ids_rows[...]
    greet([me.to(y=dy, zl=dz) for dy, dz in PEERS] + [right, left, core, far])
    links = Links(send_sem, recv_sem)
    own, far_e = me.expert(0, 0), me.expert(0, 1)

    from_far = links.send(w_in, w.at[own, me.c], far)
    from_left0 = links.send(w_in, w.at[own, me.c], right)
    from_right0 = links.send(w_in, w.at[own, me.c], left)
    from_core = {(0, 0): [links.send(w_in, w.at[own, me.c], core)]}

    def cut(array, y, zl):
        return array.at[:, me.columns(y, zl)]

    plane = [
        links.send(cut(tok, 2, 0), l_tok.at[0], up),
        links.send(cut(og, 2, 0), r_og.at[0], down),
    ]
    z_in = {}
    z_in[2, 0] = links.send(cut(tok, 2, 1), z_tok.at[2], pair)
    z_in[2, 1] = links.send(cut(og, 2, 1), z_og.at[2], pair)
    near = []
    for y, device in ((1, up), (3, down)):
        near.append(links.send(cut(tok, y, 0), x.at[me.b], device))
        near.append(links.send(cut(og, y, 0), g.at[me.b], device))
    for y in (1, 3):
        z_in[y, 0] = links.send(cut(tok, y, 1), z_tok.at[y], pair)
        z_in[y, 1] = links.send(cut(og, y, 1), z_og.at[y], pair)
    z_in[0, 0] = links.send(cut(tok, 0, 1), x.at[me.b], pair)
    z_in[0, 1] = links.send(cut(og, 0, 1), g.at[me.b], pair)
    names = [links.send(ids, ids_in.at[me.b], me.to(y=dy, zl=dz)) for dy, dz in PEERS]
    local = [
        pltpu.make_async_copy(w_in, w.at[own, me.c], own_sem.at[0]),
        pltpu.make_async_copy(cut(tok, 0, 0), x.at[me.b], own_sem.at[1]),
        pltpu.make_async_copy(cut(og, 0, 0), g.at[me.b], own_sem.at[2]),
        pltpu.make_async_copy(ids, ids_in.at[me.b], own_sem.at[3]),
    ]
    for copy in local:
        copy.start()

    @pl.loop(0, 64)
    def _(i):
        part[i // 8, pl.ds(pl.multiple_of(i % 8 * 32, 32), 32), :] = jnp.zeros((32, 768), BF16)

    def pass_on(expert, device, rows=pl.ds(0, 384)):
        piece = w.at[expert, me.c, rows, :]
        return links.send(piece, piece, device)

    low, high = pl.ds(0, 192), pl.ds(192, 192)
    across, ends = [], []
    z_in[2, 0].wait_recv()
    across.append(links.send(z_tok.at[2], l_tok.at[1], up))
    plane[0].wait_recv()
    ends.append(links.send(l_tok.at[0], x.at[me.block(3, 0)], up))
    z_in[2, 1].wait_recv()
    across.append(links.send(z_og.at[2], r_og.at[1], down))
    plane[1].wait_recv()
    ends.append(links.send(r_og.at[0], g.at[me.block(1, 0)], down))
    halves = {0: [], 1: []}

    def sideways(dz, from_left, from_right):
        from_left.wait_recv()
        halves[dz].append(pass_on(me.expert(3, dz), right, low))
        from_core[3, dz] = [pass_on(me.expert(3, dz), core)]
        from_right.wait_recv()
        halves[dz].append(pass_on(me.expert(1, dz), left, high))
        from_core[1, dz] = [pass_on(me.expert(1, dz), core)]

    sideways(0, from_left0, from_right0)
    late = []

    def partner(y, device):
        z_in[y, 0].wait_recv()
        late.append(links.send(z_tok.at[y], x.at[me.block(0, 1)], device))
        z_in[y, 1].wait_recv()
        late.append(links.send(z_og.at[y], g.at[me.block(0, 1)], device))

    from_far.wait_recv()
    from_left1 = pass_on(far_e, right)
    from_right1 = pass_on(far_e, left)
    from_core[0, 1] = [pass_on(far_e, core)]
    partner(1, up)
    partner(3, down)
    across[0].wait_recv()
    late.append(links.send(l_tok.at[1], x.at[me.block(3, 1)], up))
    across[1].wait_recv()
    late.append(links.send(r_og.at[1], g.at[me.block(1, 1)], down))

    def second(dz):
        from_core[2, dz] = []
        for n, half in enumerate(halves[dz]):
            half.wait_recv()
            from_core[2, dz].append(pass_on(me.expert(2, dz), core, (low, high)[n]))

    def turn(dz):
        for y in range(4):
            b = me.block(y, dz)
            at = pl.ds(pl.multiple_of(b * 128, 128), 128)
            xt[:, at] = jnp.transpose(x[b])
            ogt[:, at] = jnp.transpose(g[b])

    def name_rows(dz):
        for y in range(4):
            b = me.block(y, dz)
            at = pl.ds(pl.multiple_of(b * 128, 128), 128)
            idc[at, :] = jnp.transpose(ids_in[b])

    def keep(step, dz):
        for copy in from_core[step, dz]:
            copy.wait_recv()
        e = me.expert(step, dz)
        pltpu.make_async_copy(w.at[e], w_out.at[e], w_sem.at[e]).start()

    def product(e, dz):
        plane_at = pl.multiple_of((me.zl + dz) % 2 * 4, 4)
        for n, source in ((0, x), (1, x), (2, g)):
            cols = slice(n * 256, n * 256 + 256)
            rows = source[pl.ds(plane_at, 4)].reshape(512, 768)
            out = jnp.dot(rows, w[e, :, :, cols].reshape(768, 256), preferred_element_type=F32)
            for y in range(4):
                names_at = pl.ds(pl.multiple_of((plane_at + y) * 128, 128), 128)
                for k in range(2):
                    here = part.at[plane_at + y, k * 128 : k * 128 + 128, cols]
                    chosen = idc[names_at, k : k + 1] == e
                    old = here[...].astype(F32)
                    here[...] = jnp.where(chosen, out[y * 128 : y * 128 + 128], old).astype(BF16)

    def first_six(i):
        g2 = i // 2
        step = (g2 + 1) // 2 * (1 + 2 * (i % 2))
        return me.expert(step, (1 - (g2 + 1) // 2) * (i % 2) + g2 // 2)

    for copy in near + ends + names:
        copy.wait_recv()
    for copy in local:
        copy.wait()
    turn(0)
    name_rows(0)
    for step, dz in ((0, 0), (0, 1), (1, 0), (3, 0)):
        keep(step, dz)

    @pl.loop(0, 4)
    def _(i):
        product(first_six(i), 0)

    second(0)
    sideways(1, from_left1, from_right1)
    keep(1, 1)
    keep(3, 1)

    @pl.loop(4, 6)
    def _(i):
        product(first_six(i), 0)

    for copy in [z_in[0, 0], z_in[0, 1]] + late:
        copy.wait_recv()
    name_rows(1)

    @pl.loop(0, 6)
    def _(i):
        product(first_six(i), 1)

    second(1)
    keep(2, 0)
    keep(2, 1)

    @pl.loop(0, 2)
    def _(i):
        product(me.expert(2, i), 0)

    opened = {0: open_sums(me, links, part, 0, sums)}

    @pl.loop(0, 2)
    def _(i):
        product(me.expert(2, i), 1)

    close_sums(me, links, part, weight_rows, h_out, opened, sums, lambda: turn(1))
    links.finish()
    for e in range(8):
        pltpu.make_async_copy(w.at[e], w_out.at[e], w_sem.at[e]).wait()


def forward(tokens, out_grad, ids, weight, w_gate, w_up, w_down):
    vmem, anywhere = pl.BlockSpec(memory_space=pltpu.VMEM), pl.BlockSpec(memory_space=pl.ANY)
    blocks = lambda n: pltpu.VMEM((n, 128, 768), BF16)
    rows = lambda *shape: pltpu.VMEM(shape + (768,), BF16)
    return pl.pallas_call(
        forward_kernel,
        out_shape=(
            jax.ShapeDtypeStruct((8, 256, 768), BF16),
            jax.ShapeDtypeStruct((768, 1024), BF16),
            jax.ShapeDtypeStruct((768, 1024), BF16),
            jax.ShapeDtypeStruct((1024, 8), jnp.int32),
            jax.ShapeDtypeStruct((8, 2, 384, 768), BF16),
        ),
        in_specs=[vmem] * 7,
        out_specs=(anywhere,) + (vmem,) * 3 + (anywhere,),
        scratch_shapes=[
            pltpu.VMEM((8, 256, 768), BF16),
            pltpu.VMEM((384, 768), BF16),
            pltpu.VMEM((8, 128), jnp.int32),
            blocks(8),
            blocks(8),
            pltpu.VMEM((8, 8, 128), jnp.int32),
            pltpu.VMEM((8, 2, 384, 768), BF16),
            blocks(4),
            blocks(4),
            blocks(2),
            blocks(2),
            pltpu.SemaphoreType.DMA((FORWARD_COPIES,)),
            pltpu.SemaphoreType.DMA((FORWARD_COPIES,)),
            pltpu.SemaphoreType.DMA((4,)),
            pltpu.SemaphoreType.DMA((8,)),
            pltpu.VMEM((8, 128), F32),
            pltpu.VMEM((128, 8), F32),
        ]
        + [rows(2, 64)] * 4
        + [rows(2, 128)] * 2
        + [rows(128)] * 2
        + [rows(4, 128), rows(128)]
        + [rows(64)] * 6
        + [rows(128)] * 2
        + [rows(256), pltpu.SemaphoreType.DMA((2,))],
        compiler_params=pltpu.CompilerParams(collective_id=0, has_side_effects=True, vmem_limit_bytes=60 << 20),
        name="forward",
    )(tokens, out_grad, ids, weight, w_gate, w_up, w_down)


FINISH_COPIES = 8 + 4 + 4 + 4 + 1 + 16


def finish_kernel(
    xt_in, ogt_in, ids_in, h_in, w, d_out, gate_out, up_out, down_out,
    xt, ogt, ids, h, w_all, he, g, cr, dx, g_out, zd, dl, dr, a2, ra, rb, sa, sb, oa, ob, fl, fr, zs, zr,
    send_sem, recv_sem, w_sem, own_sem,
):
    me = Spot()
    right, left, core, far = me.to(x=1), me.to(x=3), me.to(c=1), me.to(zh=1)
    up, down, pair = me.to(y=1), me.to(y=3), me.to(zl=1)
    sources = ((ids_in, ids), (h_in, h), (xt_in, xt), (ogt_in, ogt))
    heads = [pltpu.make_async_copy(src, dst, w_sem.at[8 + n]) for n, (src, dst) in enumerate(sources)]
    loads = [pltpu.make_async_copy(w.at[e], w_all.at[e], w_sem.at[e]) for e in range(8)]
    for load in heads + loads:
        load.start()
    greet([up, down, pair, right, left, core, far])
    links = Links(send_sem, recv_sem)
    low, high = pl.ds(0, 192), pl.ds(192, 192)
    mine, others = me.c, 1 - me.c
    swapped, first_a, first_b, other_b, other_a, last_a, last_b = {}, {}, {}, {}, {}, {}, {}

    def fill(step, dz):
        e = me.expert(step, dz)

        @pl.loop(0, 8)
        def _(q):
            at = pl.ds(pl.multiple_of(q * 128, 128), 128)
            chosen = [(ids[at, k : k + 1] == e).astype(F32) for k in range(2)]
            m0, m1 = [jnp.broadcast_to(m, (128, 128)).astype(BF16) for m in chosen]
            for n in range(6):
                cols = slice(n * 128, n * 128 + 128)
                he[e, at, cols] = h[q, :128, cols] * m0 + h[q, 128:, cols] * m1

    def product(step, dz):
        e = me.expert(step, dz)
        for n, left_t in ((0, xt), (1, xt), (2, ogt)):
            cols = slice(n * 256, n * 256 + 256)
            out = jnp.dot(left_t[...], he[e, :, cols], preferred_element_type=F32).astype(BF16)
            g[e, 0, :, cols] = out[:384]
            g[e, 1, :, cols] = out[384:]
        swapped[step, dz] = links.send(g.at[e, others], cr.at[e], core)

    def start_far(dz):
        e = me.expert(2, dz)
        swapped[2, dz].wait_recv()
        add_rows(a2.at[dz], [g.at[e, mine], cr.at[e]], 384)
        first_a[dz] = links.send(a2.at[dz, low, :], ra.at[dz], right)
        first_b[dz] = links.send(a2.at[dz, high, :], rb.at[dz], left)

    def start_near(dz):
        e = me.expert(1, dz)
        swapped[1, dz].wait_recv()
        add_rows(ob.at[dz], [g.at[e, mine, high, :], cr.at[e, high, :]], 192)
        other_b[dz] = links.send(ob.at[dz], fl.at[dz, high, :], right)
        e = me.expert(3, dz)
        swapped[3, dz].wait_recv()
        add_rows(oa.at[dz], [g.at[e, mine, low, :], cr.at[e, low, :]], 192)
        other_a[dz] = links.send(oa.at[dz], fr.at[dz, low, :], left)

    def relay(dz):
        e = me.expert(1, dz)
        first_a[dz].wait_recv()
        add_rows(sa.at[dz], [g.at[e, mine, low, :], cr.at[e, low, :], ra.at[dz]], 192)
        last_a[dz] = links.send(sa.at[dz], fl.at[dz, low, :], right)
        e = me.expert(3, dz)
        first_b[dz].wait_recv()
        add_rows(sb.at[dz], [g.at[e, mine, high, :], cr.at[e, high, :], rb.at[dz]], 192)
        last_b[dz] = links.send(sb.at[dz], fr.at[dz, high, :], left)

    def token_part(n):
        cols = slice(n * 256, n * 256 + 256)
        total = None
        for e in range(8):
            part = lax.dot_general(
                he[e, :, :512], w_all[e, cols, :512], (((1,), (1,)), ((), ())), preferred_element_type=F32
            )
            total = part if total is None else total + part
        for q in range(8):
            dx[q, :, cols] = total[q * 128 : q * 128 + 128].astype(BF16)

    for load in heads:
        load.wait()
    for step in (2, 1):
        fill(step, 1)
        product(step, 1)
    start_far(1)
    fill(3, 1)
    product(3, 1)
    for step, dz in ((0, 1), (0, 0), (1, 0)):
        fill(step, dz)
    start_near(1)
    for step in (2, 3):
        fill(step, 0)
    for load in loads:
        load.wait()
    token_part(0)
    token_part(1)
    relay(1)
    token_part(2)

    first, last = pl.ds(0, 64), pl.ds(64, 64)
    columns = lambda y, zl: d_out.at[:, me.columns(y, zl)]
    l_in = {0: links.send(dx.at[me.block(2, 0), first, :], dl.at[0], up)}
    r_in = {0: links.send(dx.at[me.block(2, 0), last, :], dr.at[0], down)}
    z_in = {y: links.send(dx.at[me.block(y, 1)], zd.at[y], pair) for y in (2, 1, 3)}
    back = [
        links.send(dx.at[me.block(0, 1)], columns(0, 0), pair),
        links.send(dx.at[me.block(1, 0)], columns(0, 0), up),
        links.send(dx.at[me.block(3, 0)], columns(0, 0), down),
    ]
    keep = pltpu.make_async_copy(dx.at[me.b], columns(0, 0), own_sem)
    keep.start()

    def hand_on(dz):
        l_in[dz].wait_recv()
        back.append(links.send(dl.at[dz], d_out.at[first, me.columns(3, dz)], up))
        r_in[dz].wait_recv()
        back.append(links.send(dr.at[dz], d_out.at[last, me.columns(1, dz)], down))

    product(2, 0)
    product(1, 0)
    start_far(0)
    product(3, 0)
    z_in[2].wait_recv()
    l_in[1] = links.send(zd.at[2, first, :], dl.at[1], up)
    r_in[1] = links.send(zd.at[2, last, :], dr.at[1], down)
    hand_on(0)
    start_near(0)
    product(0, 1)
    z_in[1].wait_recv()
    back.append(links.send(zd.at[1], columns(0, 1), up))
    for group in (other_b, other_a, last_a, last_b):
        group[1].wait_recv()
    e = me.expert(0, 1)
    swapped[0, 1].wait_recv()
    add_rows(zs, [g.at[e, mine], cr.at[e], fl.at[1], fr.at[1]], 384)
    cross = links.send(zs, zr, far)
    z_in[3].wait_recv()
    back.append(links.send(zd.at[3], columns(0, 1), down))
    relay(0)
    product(0, 0)
    hand_on(1)
    for group in (other_b, other_a, last_a, last_b):
        group[0].wait_recv()
    swapped[0, 0].wait_recv()
    cross.wait_recv()
    e = me.expert(0, 0)
    add_rows(g_out, [g.at[e, mine], cr.at[e], fl.at[0], fr.at[0], zr], 384)
    gate_out[...] = g_out[:, :256]
    up_out[...] = g_out[:, 256:512]
    down_out[...] = jnp.transpose(g_out[:, 512:])
    for copy in back:
        copy.wait_recv()
    keep.wait()
    links.finish()


def finish(xt, ogt, ids, h, w):
    vmem, anywhere = pl.BlockSpec(memory_space=pltpu.VMEM), pl.BlockSpec(memory_space=pl.ANY)
    half, full = pltpu.VMEM((2, 192, 768), BF16), pltpu.VMEM((2, 384, 768), BF16)
    one = pltpu.VMEM((384, 768), BF16)
    return pl.pallas_call(
        finish_kernel,
        out_shape=(
            jax.ShapeDtypeStruct((128, 6144), BF16),
            jax.ShapeDtypeStruct((384, 256), F32),
            jax.ShapeDtypeStruct((384, 256), F32),
            jax.ShapeDtypeStruct((256, 384), F32),
        ),
        in_specs=[anywhere] * 5,
        out_specs=(anywhere,) + (vmem,) * 3,
        scratch_shapes=[
            pltpu.VMEM((768, 1024), BF16),
            pltpu.VMEM((768, 1024), BF16),
            pltpu.VMEM((1024, 8), jnp.int32),
            pltpu.VMEM((8, 256, 768), BF16),
            pltpu.VMEM((8, 768, 768), BF16),
            pltpu.VMEM((8, 1024, 768), BF16),
            pltpu.VMEM((8, 2, 384, 768), BF16),
            pltpu.VMEM((8, 384, 768), BF16),
            pltpu.VMEM((8, 128, 768), BF16),
            pltpu.VMEM((384, 768), F32),
            pltpu.VMEM((4, 128, 768), BF16),
            pltpu.VMEM((2, 64, 768), BF16),
            pltpu.VMEM((2, 64, 768), BF16),
        ]
        + [full] + [half] * 6 + [full] * 2 + [one] * 2
        + [
            pltpu.SemaphoreType.DMA((FINISH_COPIES,)),
            pltpu.SemaphoreType.DMA((FINISH_COPIES,)),
            pltpu.SemaphoreType.DMA((12,)),
            pltpu.SemaphoreType.DMA,
        ],
        compiler_params=pltpu.CompilerParams(collective_id=2, has_side_effects=True, vmem_limit_bytes=60 << 20),
        name="finish",
    )(xt, ogt, ids, h, w)


def deliver_kernel(*refs):
    sources, results, places = refs[:4], refs[4:8], refs[8:12]
    in_sem, out_sem = refs[12:]
    pieces = []
    for n in range(4):
        rows = sources[n].shape[0]
        step = 32 if n == 0 else rows
        for row in range(0, rows, step):
            pieces.append((n, pl.ds(row, step)))
    fetch = [pltpu.make_async_copy(sources[n].at[at], places[n].at[at], in_sem.at[i]) for i, (n, at) in enumerate(pieces)]
    store = [pltpu.make_async_copy(places[n].at[at], results[n].at[at], out_sem.at[i]) for i, (n, at) in enumerate(pieces)]
    for copy in fetch:
        copy.start()
    for first, second in zip(fetch, store):
        first.wait()
        second.start()
    for copy in store:
        copy.wait()


def deliver(*arrays):
    anywhere = pl.BlockSpec(memory_space=pl.ANY)
    return pl.pallas_call(
        deliver_kernel,
        out_shape=tuple(jax.ShapeDtypeStruct(a.shape, a.dtype) for a in arrays),
        in_specs=[anywhere] * 4,
        out_specs=(anywhere,) * 4,
        scratch_shapes=[pltpu.VMEM(a.shape, a.dtype) for a in arrays]
        + [pltpu.SemaphoreType.DMA((7,)), pltpu.SemaphoreType.DMA((7,))],
        name="deliver",
    )(*arrays)


def shards(tokens, out_grad, expert_ids, route_weight, w_gate, w_up, w_down):
    ids, weight = jnp.transpose(expert_ids), jnp.transpose(route_weight)
    h, xt, ogt, names, w = forward(tokens, out_grad, ids, weight, w_gate[0], w_up[0], w_down[0])
    d_tokens, gate, up, down = deliver(*finish(xt, ogt, names, h, w.reshape(8, 768, 768)))
    return d_tokens, gate[None], up[None], down[None]


def solution(mesh):
    in_specs = (
        P(("dp", "ep"), None),
        P(("dp", "ep"), None),
        P(("dp", "ep"), None),
        P(("dp", "ep"), None),
        P("ep", "dp", None),
        P("ep", "dp", None),
        P("ep", None, "dp"),
    )
    out_specs = (
        P(("dp", "ep"), None),
        P("ep", "dp", None),
        P("ep", "dp", None),
        P("ep", None, "dp"),
    )
    return jax.shard_map(shards, mesh=mesh, in_specs=in_specs, out_specs=out_specs, check_vma=False)
```
